128 devices in a mesh: grp: 8 (over x, core), dev: 16 (over z, y).
Axes of the slice: x: 4, y: 4, z: 4, core: 2. Of those that a mesh axis runs over, the one named last changes fastest.
Arguments:
- transition: float32 [256, 256, 256], P(('grp', 'dev')), as said below
- observe: float32 [256, 64, 256], P(('grp', 'dev')), may hold values from -0.375 to 0.375
- noise_obs: float32 [256, 64], P(('grp', 'dev')), may hold values from 100 to 1000
- measured: float32 [256, 64], P(('grp', 'dev')), may hold values from -60 to 60
- noise_state: float32 [256, 256], replicated, as said below
- prior_mean: float32 [256], replicated, may hold values from -6 to 6
- prior_cov: float32 [256, 256], replicated, as said below
Outputs:
- means: float32 [256, 256], P(('grp', 'dev'))
- covs: float32 [256, 256, 256], P(('grp', 'dev'))
The draws below stay inside these ranges and needn't reach their ends.
Inputs may be any that keep to these rules, and one draw needn't show every extreme that they name: `transition`: each matrix is (I + G) / sqrt(1.0625) with G of independent entries of deviation 0.25 / sqrt(256). `noise_state`: symmetric positive definite, 0.001 (I + E) with E symmetric of spectral norm well under one. `prior_cov`: symmetric positive definite, I + E with E symmetric of spectral norm well under one.
All inputs are finite; a program needn't handle non-finite values.
Results may differ from the reference program's by a relative error of at most 0.0003.
Values sent between devices are 32-bit elements; how exact they have to be, the bound alone decides.
No kernel may reach another device: no remote copies, remote signals or barrier semaphores. Data moves between devices by JAX's collectives and lax.ppermute only.
A program may use at most 128 MiB of HBM per device.

```python
import math
import jax
import jax.numpy as jnp
from jax import lax

NS = 256
NO = 64
STEPS = 256


def draw_transition(key, part):
    noise = jax.random.normal(key, (STEPS, NS, NS), jnp.float32) * (0.25 / jnp.sqrt(jnp.float32(NS)))
    return (jnp.eye(NS, dtype=jnp.float32)[None] + noise) / jnp.sqrt(jnp.float32(1.0625))


def symmetric_part(key):
    base = jax.random.normal(key, (NS, NS), jnp.float32) / jnp.sqrt(jnp.float32(NS))
    return 0.3 * (base + base.T) / jnp.sqrt(jnp.float32(2.0))


def draw_noise_state(key, part):
    return 0.001 * (jnp.eye(NS, dtype=jnp.float32) + symmetric_part(jax.random.fold_in(key, 11)))


def draw_prior_cov(key, part):
    return jnp.eye(NS, dtype=jnp.float32) + symmetric_part(jax.random.fold_in(key, 23))


def shard_levels(stream_key, shape, pieces, least, largest):
    def one(axis_at, shards_of):
        steps = jax.random.uniform(jax.random.fold_in(jax.random.fold_in(stream_key, 6), axis_at), (shards_of,), jnp.float32, least / len(pieces), largest / len(pieces))
        return jnp.repeat(jnp.exp(steps), shape[axis_at] // shards_of).reshape((-1,) + (1,) * (len(shape) - axis_at - 1))

    factor_of = one(*pieces[0])
    for cut in pieces[1:]:
        factor_of = factor_of * one(*cut)
    return factor_of


def centred(key, dims, spread, bound, split=(), kind=jnp.bfloat16):
    drawn = spread * jax.random.normal(key, dims, jnp.float32)
    if split:
        drawn = drawn * shard_levels(key, dims, split, -0.22, 0.18)
    return jnp.clip(drawn, -bound, bound).astype(kind)


def setup_inputs(seed: int = 0) -> dict:
    streams_of = jax.random.split(jax.random.key(seed), 8)
    transition = draw_transition(jax.random.fold_in(streams_of[7], 71), 0)
    observe = centred(streams_of[1], (STEPS, NO, NS), NS ** -0.5, 0.375, ((0, 128),), jnp.float32)
    noise_obs = jnp.clip(jnp.exp(math.log(1000.0) - 2.3025851 * jax.random.uniform(streams_of[2], (STEPS, NO), jnp.float32) ** shard_levels(streams_of[2], (STEPS, NO), ((0, 128),), -0.2, 0.2)), 100.0, 1000.0)
    measured = centred(streams_of[3], (STEPS, NO), 10.0, 60.0, ((0, 128),), jnp.float32)
    noise_state = draw_noise_state(jax.random.fold_in(streams_of[7], 71), 0)
    prior_mean = centred(streams_of[5], (NS,), 1.0, 6.0, (), jnp.float32)
    prior_cov = draw_prior_cov(jax.random.fold_in(streams_of[7], 71), 0)
    return {"transition": transition, "observe": observe, "noise_obs": noise_obs, "measured": measured, "noise_state": noise_state, "prior_mean": prior_mean, "prior_cov": prior_cov}


def reference(transition, observe, noise_obs, measured, noise_state, prior_mean, prior_cov):
    high = lax.Precision.HIGHEST

    def advance(carry, item):
        mean, cov = carry
        forward, sensor, variance, value = item
        mean = jnp.dot(forward, mean, precision=high)
        cov = jnp.dot(jnp.dot(forward, cov, precision=high), forward.T, precision=high) + noise_state
        sensed = jnp.dot(sensor, cov, precision=high)
        innovation = jnp.dot(sensed, sensor.T, precision=high) + jnp.diag(variance)
        gain_rows = jnp.linalg.solve(innovation, sensed)
        mean = mean + jnp.dot(gain_rows.T, value - jnp.dot(sensor, mean, precision=high), precision=high)
        cov = cov - jnp.dot(sensed.T, gain_rows, precision=high)
        return ((mean, cov), (mean, cov))
    _, (means, covs) = lax.scan(advance, (prior_mean, prior_cov), (transition, observe, noise_obs, measured))
    return (means, covs)
```

```python
import functools

import jax
import jax.numpy as jnp
from jax import lax
from jax.experimental import pallas as pl
from jax.experimental.pallas import tpu as pltpu
from jax.sharding import Mesh
from jax.sharding import PartitionSpec as P


AXES = ("x", "c", "z", "y")
N = 256
O = 64
V = 16
ROWS = 2 * N + V
TOL = 1e-6
F32 = jnp.float32
BF16 = jnp.bfloat16


def split(x):
    high = x.astype(BF16)
    low = (x - high.astype(F32)).astype(BF16)
    return high, low


def dot3(a, b, dims=((1,), (0,))):
    def one(p, q):
        return lax.dot_general(p, q, (dims, ((), ())), preferred_element_type=F32)

    return one(a[0], b[0]) + (one(a[0], b[1]) + one(a[1], b[0]))


def rows(*parts):
    return tuple(jnp.concatenate([p[i] for p in parts], axis=0) for i in range(2))


def row_col(n):
    return (
        lax.broadcasted_iota(jnp.int32, (n, n), 0),
        lax.broadcasted_iota(jnp.int32, (n, n), 1),
    )


def resolvents(coupled, stacks):
    n = coupled[0].shape[0]
    row, col = row_col(n)
    eye = jnp.where(row == col, 1.0, 0.0).astype(F32)
    rate = jnp.float32(0.0)
    for each, stack in zip(coupled, stacks):
        size = jnp.abs(each)
        bound = jnp.minimum(
            jnp.max(jnp.sum(size, axis=0, keepdims=True)), jnp.sqrt(jnp.sum(size * size))
        )
        scale = 2.0 / (2.0 + bound)
        error = eye - scale * (eye + each)
        stack[0:n, :] = scale * (eye + error)
        stack[n:, :] = error
        rate = jnp.maximum(rate, jnp.minimum(bound * scale * 0.5, 0.9999998))

    @pl.when(rate * rate > TOL)
    def _():
        for stack in stacks:
            factor = split(stack[n:, :])
            stack[n:, :] = dot3(factor, factor)

    def sweep(rate):
        for stack in stacks:
            both = split(stack[...])
            fresh = dot3(both, (both[0][n:], both[1][n:]))
            stack[0:n, :] = stack[0:n, :] + fresh[0:n]
            stack[n:, :] = fresh[n:]
        return rate * rate

    lax.while_loop(lambda rate: rate > TOL, sweep, rate * rate)
    return [stack[0:n, :] for stack in stacks]


def unpack(ref):
    move = ref[0:N, :]
    both = ref[N : 2 * N, :]
    vecs = ref[2 * N :, :]
    row, col = row_col(N)
    turned = both.T
    spread = jnp.where(row <= col, both, turned)
    info = jnp.where(row == col, vecs[2:3, :], jnp.where(row > col, both, turned))
    return move, spread, info, vecs


def pack(ref, move, spread, info, offset, info_vec):
    row, col = row_col(N)
    ref[0:N, :] = move
    ref[N : 2 * N, :] = jnp.where(row <= col, spread, info)
    diag = jnp.sum(jnp.where(row == col, info, 0.0), axis=0, keepdims=True)
    place = lax.broadcasted_iota(jnp.int32, (V, N), 0)
    ref[2 * N :, :] = jnp.where(
        place == 0, offset, jnp.where(place == 1, info_vec, jnp.where(place == 2, diag, 0.0))
    )


def combine(firsts, seconds, stacks):
    pairs = []
    for (move_a, spr_a, mat_a, vecs_a), (move_b, spr_b, mat_b, vecs_b) in zip(firsts, seconds):
        move_a2, spr_a2, mat_b2 = split(move_a), split(spr_a), split(mat_b)
        up = dot3(rows(mat_b2, split(vecs_b)), spr_a2)
        seen = dot3(rows(move_a2, split(vecs_a)), mat_b2)
        pairs.append((up, seen, move_a2, spr_a2))
    settled = resolvents([pair[0][0:N] for pair in pairs], stacks)
    out = []
    for first, second, pair, settle in zip(firsts, seconds, pairs, settled):
        up, seen, move_a2, spr_a2 = pair
        move_b, spr_b, _, vecs_b = second
        _, _, mat_a, vecs_a = first
        row_r = vecs_a + up[N + 1 : N + 2]
        row_s = vecs_b[1:2] - seen[N : N + 1]
        third2 = split(dot3(rows(move_a2, spr_a2, split(row_r)), split(settle)))
        fourth = dot3(third2, split(move_b))
        back2 = (third2[0][0:N], third2[1][0:N])
        fifth = dot3(
            rows(split(seen[0:N]), split(jnp.broadcast_to(row_s, (V, N)))), back2, ((1,), (1,))
        )
        spread = dot3(split(move_b.T), split(fourth[N : 2 * N])) + spr_b
        out.append(
            (
                fourth[0:N],
                spread,
                fifth[0:N] + mat_a,
                fourth[2 * N : 2 * N + 1] + vecs_b[0:1],
                fifth[N : N + 1] + vecs_a[1:2],
            )
        )
    return out


def apply_state(mean, cov, seconds, stacks):
    cov2 = split(cov)
    ups = [dot3(rows(split(mat_b), split(vecs_b)), cov2) for _, _, mat_b, vecs_b in seconds]
    settled = resolvents([up[0:N] for up in ups], stacks)
    out = []
    for (move_b, spr_b, _, vecs_b), up, settle in zip(seconds, ups, settled):
        row_r = mean + up[N + 1 : N + 2]
        third = dot3(rows(cov2, split(row_r)), split(settle))
        fourth = dot3(split(third), split(move_b))
        spread = dot3(split(move_b.T), split(fourth[0:N])) + spr_b
        out.append((fourth[N:] + vecs_b[0:1], spread))
    return out


def build_kernel(
    trans_in, obs_in, noise_in, meas_in, state_in, two_ref, pair, trans, obs, noise, meas,
    noise_state, sems, stack, small_a, small_b,
):
    copies = [
        pltpu.make_async_copy(source, target, sems.at[k])
        for k, (source, target) in enumerate(
            (
                (obs_in, obs),
                (state_in, noise_state),
                (trans_in, trans),
                (noise_in, noise),
                (meas_in, meas),
            )
        )
    ]
    for copy in copies:
        copy.start()
    for copy in copies:
        copy.wait()
    state = noise_state[...]
    state2 = split(state)
    place = lax.broadcasted_iota(jnp.int32, (V, N), 0)
    row, col = row_col(O)
    parts = []
    for k in range(2):
        sensor2 = split(obs[k])
        sensed = dot3(sensor2, state2)
        seen = dot3(sensor2, split(trans[k]))
        inner = dot3(split(sensed), sensor2, ((1,), (1,)))
        variance = noise[k : k + 1, :]
        root = lax.rsqrt(variance)
        root = root * (1.5 - 0.5 * variance * root * root)
        root_col = jnp.sum(jnp.where(row == col, root, 0.0), axis=1, keepdims=True)
        parts.append((sensed, seen, root_col * inner * root, root, root_col))
    inverses = resolvents([part[2] for part in parts], (small_a, small_b))
    steps = []
    for k in range(2):
        sensed, seen, _, root, root_col = parts[k]
        inverse2 = split(root_col * inverses[k] * root)
        pair2 = split(jnp.concatenate([seen, sensed], axis=1))
        solved = dot3(inverse2, pair2)
        value = split(jnp.broadcast_to(meas[k : k + 1, :], (V, O)))
        vec = dot3(split(dot3(value, inverse2)), pair2)
        turned2 = split(jnp.concatenate([seen.T, sensed.T], axis=0))
        full = dot3(turned2, split(solved))
        vecs = jnp.where(place == 0, vec[0:1, N:], jnp.where(place == 1, vec[0:1, 0:N], 0.0))
        steps.append((trans[k].T - full[0:N, N:], state - full[N:, N:], full[0:N, 0:N], vecs))
    move, spread, info, vecs = steps[0]
    pack(pair.at[0], move, spread, info, vecs[0:1], vecs[1:2])
    pack(two_ref, *combine(steps[0:1], steps[1:2], [stack])[0])
    pair[1] = two_ref[...]


def upper(here, axis, step):
    shift = {"x": 5, "c": 4, "z": 2, "y": 0}[axis] + step // 2
    return ((here[0] >> shift) & 1) == 1


def order(flag, mine, theirs, first, second):
    first[...] = jnp.where(flag, theirs[...], mine[...])
    second[...] = jnp.where(flag, mine[...], theirs[...])
    return unpack(first), unpack(second)


def total_kernel(axis, step, here, mine, theirs, after, out, first, second, stack):
    a, b = order(upper(here, axis, step), mine, theirs, first, second)
    pack(out, *combine([a], [b], [stack])[0])


def core_kernel(here, mine, theirs, after, out, half, first, second, stack):
    total_kernel("c", 1, here, mine, theirs, after, out, first, second, stack)
    half[...] = jnp.where(upper(here, "c", 1), out[HALF:, :], out[0:HALF, :])


def slow_kernel(axis, step, here, theirs, pair, after, out, stack):
    flag = upper(here, axis, step)

    @pl.when(flag)
    def _():
        def one(k, carry):
            pack(out.at[k], *combine([unpack(theirs)], [unpack(pair.at[k])], [stack])[0])
            return carry

        lax.fori_loop(0, 2, one, 0)

    @pl.when(jnp.logical_not(flag))
    def _():
        out[...] = pair[...]


def merge_kernel(here, late, early, after, out, stack):
    z_up, c_up = upper(here, "z", 2), upper(here, "c", 1)

    @pl.when(jnp.logical_and(z_up, c_up))
    def _():
        pack(out, *combine([unpack(late)], [unpack(early)], [stack])[0])

    @pl.when(jnp.logical_not(z_up))
    def _():
        out[...] = late[...]

    @pl.when(jnp.logical_not(c_up))
    def _():
        out[...] = early[...]


def steps_kernel(here, theirs, low, pair, after, out, whole, stack, stack_b):
    x_up = upper(here, "x", 1)
    held = jnp.logical_or(upper(here, "z", 2), upper(here, "c", 1))

    @pl.when(jnp.logical_and(x_up, held))
    def _():
        pack(whole, *combine([unpack(theirs)], [unpack(low)], [stack])[0])

    @pl.when(jnp.logical_not(x_up))
    def _():
        whole[...] = low[...]

    @pl.when(jnp.logical_not(held))
    def _():
        whole[...] = theirs[...]

    @pl.when(jnp.logical_or(x_up, held))
    def _():
        first = unpack(whole)
        done = combine(
            [first, first], [unpack(pair.at[0]), unpack(pair.at[1])], [stack, stack_b]
        )
        pack(out.at[0], *done[0])
        pack(out.at[1], *done[1])

    @pl.when(jnp.logical_not(jnp.logical_or(x_up, held)))
    def _():
        out[...] = pair[...]


def prior_kernel(whole, mean, cov, mean_out, cov_out, stack):
    state = jnp.broadcast_to(mean[...], (V, N))
    mean_out[...], cov_out[...] = apply_state(state, cov[...], [unpack(whole)], [stack])[0]


HN = N // 2


def second_kernel(here, mine, other, mean, cov, after, theirs, out, stack):
    flag = upper(here, "c", 1)
    theirs[0:HALF, :] = jnp.where(flag, other[...], mine[...])
    theirs[HALF:, :] = jnp.where(flag, mine[...], other[...])
    mean_b, cov_b = apply_state(mean[...], cov[...], [unpack(theirs)], [stack])[0]
    row, col = row_col(HN)
    last = cov_b[HN:, HN:]
    out[0:HN, 0:HN] = jnp.where(row <= col, cov_b[0:HN, 0:HN], last)
    out[0:HN, HN:] = cov_b[0:HN, HN:]
    diag = jnp.sum(jnp.where(row == col, last, 0.0), axis=0, keepdims=True)
    out[HN : HN + 8, :] = mean_b[0:8]
    out[HN + 8 :, :] = jnp.broadcast_to(jnp.concatenate([diag, diag], axis=1), (8, N))


def final_kernel(here, state_a, state_b, mean, cov, pair, means, covs, packed, prior, stack, stack_b):
    packed[...] = jnp.where(upper(here, "x", 1), state_b[...], state_a[...])
    flag = upper(here, "x", 2)
    row, col = row_col(HN)
    mixed = packed[0:HN, 0:HN]
    turned = mixed.T
    side = packed[0:HN, HN:]
    last = jnp.where(
        row == col, packed[HN + 8 : HN + 9, 0:HN], jnp.where(row > col, mixed, turned)
    )
    prior[0:HN, 0:HN] = jnp.where(flag, jnp.where(row <= col, mixed, turned), cov[0:HN, 0:HN])
    prior[0:HN, HN:] = jnp.where(flag, side, cov[0:HN, HN:])
    prior[HN:, 0:HN] = jnp.where(flag, side.T, cov[HN:, 0:HN])
    prior[HN:, HN:] = jnp.where(flag, last, cov[HN:, HN:])
    mean_in = jnp.broadcast_to(jnp.where(flag, packed[HN : HN + 1, :], mean[...]), (V, N))
    done = apply_state(mean_in, prior[...], [unpack(pair.at[0]), unpack(pair.at[1])], [stack, stack_b])
    for k in range(2):
        means[k : k + 1, :] = done[k][0][0:1]
        covs[k] = done[k][1]


def call(kernel, places, outs, scratch, products):
    spaces = {"s": pltpu.SMEM, "v": pltpu.VMEM, "a": pl.ANY, "h": pltpu.HBM}
    vmem = pl.BlockSpec(memory_space=pltpu.VMEM)
    shapes = [jax.ShapeDtypeStruct(shape, F32) for shape in outs]
    buffers = [pltpu.VMEM(shape, F32) if isinstance(shape, tuple) else shape for shape in scratch]
    return pl.pallas_call(
        kernel,
        out_shape=shapes if len(shapes) > 1 else shapes[0],
        in_specs=[pl.BlockSpec(memory_space=spaces[place]) for place in places],
        out_specs=[vmem] * len(shapes) if len(shapes) > 1 else vmem,
        scratch_shapes=buffers,
        compiler_params=pltpu.CompilerParams(vmem_limit_bytes=24 << 20),
        cost_estimate=pl.CostEstimate(
            flops=products * 6 * N**3, transcendentals=0, bytes_accessed=8 * N * N
        ),
    )


ELEMENT = (ROWS, N)
PAIR = (2, ROWS, N)
HALF = ROWS // 2
STACK = (2 * N, N)
PACKED = (HN + 16, N)


def on_device(transition, observe, noise_obs, measured, noise_state, prior_mean, prior_cov):
    here = lax.axis_index(AXES).astype(jnp.int32)[None]
    mean = prior_mean[None]

    def swap(part, axis, step):
        size = lax.axis_size(axis)
        return lax.ppermute(part, axis, [(k, k ^ step) for k in range(size)])

    def total(axis, step, mine, theirs, after):
        kernel = functools.partial(total_kernel, axis, step)
        run = call(kernel, "svva", [ELEMENT], [ELEMENT, ELEMENT, STACK], 14)
        return run(here, mine, theirs, after)

    def slow(axis, step, theirs, pair, after):
        kernel = functools.partial(slow_kernel, axis, step)
        return call(kernel, "svva", [PAIR], [STACK], 28)(here, theirs, pair, after)

    merge = call(merge_kernel, "svva", [ELEMENT], [STACK], 14)
    steps = call(steps_kernel, "svvva", [PAIR], [ELEMENT, STACK, STACK], 42)

    inputs = [(2, N, N), (2, O, N), (2, O), (2, O), (N, N)]
    build = call(
        build_kernel,
        "hhhhh",
        [ELEMENT, PAIR],
        inputs + [pltpu.SemaphoreType.DMA((5,)), STACK, (2 * O, O), (2 * O, O)],
        30,
    )
    core = call(core_kernel, "svva", [ELEMENT, (HALF, N)], [ELEMENT, ELEMENT, STACK], 14)
    prior = call(prior_kernel, "vvv", [(V, N), (N, N)], [STACK], 14)
    second = call(second_kernel, "svvvva", [ELEMENT, PACKED], [STACK], 14)
    final = call(final_kernel, "svvvvv", [(2, N), (2, N, N)], [PACKED, (N, N), STACK, STACK], 24)

    arrays = (transition, observe, noise_obs, measured, noise_state)
    whole, pair = build(*(pltpu.with_memory_space_constraint(a, pltpu.HBM) for a in arrays))
    y1 = swap(whole, "y", 1)
    whole = total("y", 1, whole, y1, here)
    y2 = swap(whole, "y", 2)
    pair = slow("y", 1, y1, pair, here)
    whole = total("y", 2, whole, y2, pair)
    z1 = swap(whole, "z", 1)
    pair = slow("y", 2, y2, pair, here)
    whole = total("z", 1, whole, z1, pair)
    z2 = swap(whole, "z", 2)
    pair = slow("z", 1, z1, pair, here)
    whole = total("z", 2, whole, z2, pair)
    c1 = swap(whole, "c", 1)
    whole, half = core(here, whole, c1, here)
    x1 = swap(half, "x", 1)
    mean_a, cov_a = prior(whole, mean, prior_cov)
    low = merge(here, c1, z2, mean_a)
    x1_other = swap(x1, "c", 1)
    theirs, packed = second(here, x1, x1_other, mean_a, cov_a, low)
    state_a = lax.ppermute(packed, "x", [(0, 2)])
    state_b = lax.ppermute(packed, "x", [(0, 3)])
    pair = steps(here, theirs, low, pair, packed)
    return final(here, state_a, state_b, mean, prior_cov, pair)


def solution(mesh):
    split_mesh = Mesh(mesh.devices.reshape(4, 2, 4, 4), AXES)
    return jax.shard_map(
        on_device,
        mesh=split_mesh,
        in_specs=(
            P(AXES, None, None),
            P(AXES, None, None),
            P(AXES, None),
            P(AXES, None),
            P(),
            P(),
            P(),
        ),
        out_specs=(P(AXES, None), P(AXES, None, None)),
        check_vma=False,
    )
```

```python
import functools

import jax
import jax.numpy as jnp
from jax import lax
from jax.experimental import pallas as pl
from jax.experimental.pallas import tpu as pltpu
from jax.sharding import Mesh
from jax.sharding import PartitionSpec as P


AXES = ("x", "c", "z", "y")
N = 256
O = 64
V = 16
ROWS = 2 * N + V
TOL = 1e-6
F32 = jnp.float32
BF16 = jnp.bfloat16


def split(x):
    high = x.astype(BF16)
    low = (x - high.astype(F32)).astype(BF16)
    return high, low


def dot3(a, b, dims=((1,), (0,))):
    def one(p, q):
        return lax.dot_general(p, q, (dims, ((), ())), preferred_element_type=F32)

    return one(a[0], b[0]) + (one(a[0], b[1]) + one(a[1], b[0]))


def rows(*parts):
    return tuple(jnp.concatenate([p[i] for p in parts], axis=0) for i in range(2))


def row_col(n):
    return (
        lax.broadcasted_iota(jnp.int32, (n, n), 0),
        lax.broadcasted_iota(jnp.int32, (n, n), 1),
    )


def resolvents(coupled, stacks):
    n = coupled[0].shape[0]
    row, col = row_col(n)
    eye = jnp.where(row == col, 1.0, 0.0).astype(F32)
    rate = jnp.float32(0.0)
    for each, stack in zip(coupled, stacks):
        size = jnp.abs(each)
        bound = jnp.minimum(
            jnp.max(jnp.sum(size, axis=0, keepdims=True)), jnp.sqrt(jnp.sum(size * size))
        )
        scale = 2.0 / (2.0 + bound)
        error = eye - scale * (eye + each)
        stack[0:n, :] = scale * (eye + error)
        stack[n:, :] = error
        rate = jnp.maximum(rate, jnp.minimum(bound * scale * 0.5, 0.9999998))

    @pl.when(rate * rate > TOL)
    def _():
        for stack in stacks:
            factor = split(stack[n:, :])
            stack[n:, :] = dot3(factor, factor)

    def sweep(rate):
        for stack in stacks:
            both = split(stack[...])
            fresh = dot3(both, (both[0][n:], both[1][n:]))
            stack[0:n, :] = stack[0:n, :] + fresh[0:n]
            stack[n:, :] = fresh[n:]
        return rate * rate

    lax.while_loop(lambda rate: rate > TOL, sweep, rate * rate)
    return [stack[0:n, :] for stack in stacks]


def unpack(move_ref, side_ref):
    both = side_ref[0:N, :]
    vecs = side_ref[N:, :]
    row, col = row_col(N)
    turned = both.T
    spread = jnp.where(row <= col, both, turned)
    info = jnp.where(row == col, vecs[2:3, :], jnp.where(row > col, both, turned))
    return move_ref[...], spread, info, vecs


def pack(move_ref, side_ref, move, spread, info, offset, info_vec):
    row, col = row_col(N)
    move_ref[...] = move
    side_ref[0:N, :] = jnp.where(row <= col, spread, info)
    diag = jnp.sum(jnp.where(row == col, info, 0.0), axis=0, keepdims=True)
    place = lax.broadcasted_iota(jnp.int32, (V, N), 0)
    side_ref[N:, :] = jnp.where(
        place == 0, offset, jnp.where(place == 1, info_vec, jnp.where(place == 2, diag, 0.0))
    )


def parts(ref):
    return ref.at[0:N], ref.at[N:]


def combine(firsts, seconds, stacks):
    pairs = []
    for (move_a, spr_a, mat_a, vecs_a), (move_b, spr_b, mat_b, vecs_b) in zip(firsts, seconds):
        move_a2, spr_a2, mat_b2 = split(move_a), split(spr_a), split(mat_b)
        up = dot3(rows(mat_b2, split(vecs_b)), spr_a2)
        seen = dot3(rows(move_a2, split(vecs_a)), mat_b2)
        pairs.append((up, seen, move_a2, spr_a2))
    settled = resolvents([pair[0][0:N] for pair in pairs], stacks)
    out = []
    for first, second, pair, settle in zip(firsts, seconds, pairs, settled):
        up, seen, move_a2, spr_a2 = pair
        move_b, spr_b, _, vecs_b = second
        _, _, mat_a, vecs_a = first
        row_r = vecs_a + up[N + 1 : N + 2]
        row_s = vecs_b[1:2] - seen[N : N + 1]
        third2 = split(dot3(rows(move_a2, spr_a2, split(row_r)), split(settle)))
        fourth = dot3(third2, split(move_b))
        back2 = (third2[0][0:N], third2[1][0:N])
        fifth = dot3(
            rows(split(seen[0:N]), split(jnp.broadcast_to(row_s, (V, N)))), back2, ((1,), (1,))
        )
        spread = dot3(split(move_b.T), split(fourth[N : 2 * N])) + spr_b
        out.append(
            (
                fourth[0:N],
                spread,
                fifth[0:N] + mat_a,
                fourth[2 * N : 2 * N + 1] + vecs_b[0:1],
                fifth[N : N + 1] + vecs_a[1:2],
            )
        )
    return out


def apply_state(mean, cov, seconds, stacks):
    cov2 = split(cov)
    ups = [dot3(rows(split(mat_b), split(vecs_b)), cov2) for _, _, mat_b, vecs_b in seconds]
    settled = resolvents([up[0:N] for up in ups], stacks)
    out = []
    for (move_b, spr_b, _, vecs_b), up, settle in zip(seconds, ups, settled):
        row_r = mean + up[N + 1 : N + 2]
        third = dot3(rows(cov2, split(row_r)), split(settle))
        fourth = dot3(split(third), split(move_b))
        spread = dot3(split(move_b.T), split(fourth[0:N])) + spr_b
        out.append((fourth[N:] + vecs_b[0:1], spread))
    return out


def build_kernel(
    trans_in, obs_in, noise_in, meas_in, state_in, move_ref, side_ref, pair, trans, obs, noise, meas,
    noise_state, sems, stack, small_a, small_b,
):
    copies = [
        pltpu.make_async_copy(source, target, sems.at[k])
        for k, (source, target) in enumerate(
            (
                (obs_in, obs),
                (state_in, noise_state),
                (trans_in, trans),
                (noise_in, noise),
                (meas_in, meas),
            )
        )
    ]
    for copy in copies:
        copy.start()
    for copy in copies:
        copy.wait()
    state = noise_state[...]
    state2 = split(state)
    place = lax.broadcasted_iota(jnp.int32, (V, N), 0)
    row, col = row_col(O)
    found = []
    for k in range(2):
        sensor2 = split(obs[k])
        sensed = dot3(sensor2, state2)
        seen = dot3(sensor2, split(trans[k]))
        inner = dot3(split(sensed), sensor2, ((1,), (1,)))
        variance = noise[k : k + 1, :]
        root = lax.rsqrt(variance)
        root = root * (1.5 - 0.5 * variance * root * root)
        root_col = jnp.sum(jnp.where(row == col, root, 0.0), axis=1, keepdims=True)
        found.append((sensed, seen, root_col * inner * root, root, root_col))
    inverses = resolvents([part[2] for part in found], (small_a, small_b))
    steps = []
    for k in range(2):
        sensed, seen, _, root, root_col = found[k]
        inverse2 = split(root_col * inverses[k] * root)
        pair2 = split(jnp.concatenate([seen, sensed], axis=1))
        solved = dot3(inverse2, pair2)
        value = split(jnp.broadcast_to(meas[k : k + 1, :], (V, O)))
        vec = dot3(split(dot3(value, inverse2)), pair2)
        turned2 = split(jnp.concatenate([seen.T, sensed.T], axis=0))
        full = dot3(turned2, split(solved))
        vecs = jnp.where(place == 0, vec[0:1, N:], jnp.where(place == 1, vec[0:1, 0:N], 0.0))
        steps.append((trans[k].T - full[0:N, N:], state - full[N:, N:], full[0:N, 0:N], vecs))
    move, spread, info, vecs = steps[0]
    pack(*parts(pair.at[0]), move, spread, info, vecs[0:1], vecs[1:2])
    pack(move_ref, side_ref, *combine(steps[0:1], steps[1:2], [stack])[0])
    pair[1, 0:N, :] = move_ref[...]
    pair[1, N:, :] = side_ref[...]


def upper(here, axis, step):
    shift = {"x": 5, "c": 4, "z": 2, "y": 0}[axis] + step // 2
    return ((here[0] >> shift) & 1) == 1


def sort(flag, ones, others, first, second):
    for half, one, other in zip((slice(0, N), slice(N, ROWS)), ones, others):
        first[half, :] = jnp.where(flag, other[...], one[...])
        second[half, :] = jnp.where(flag, one[...], other[...])


def own_kernel(axis, here, ma, mb, pa, pb, na, nb, after, out, first, second, stack):
    odd = upper(here, axis, 1)
    for half, mine, prev, later in zip((slice(0, N), slice(N, ROWS)), (ma, mb), (pa, pb), (na, nb)):
        first[half, :] = jnp.where(odd, prev[...], mine[...])
        second[half, :] = jnp.where(odd, mine[...], later[...])
    done = combine([unpack(*parts(first))], [unpack(*parts(second))], [stack])
    pack(*parts(out), *done[0])


def ring_kernel(axis, here, own, pa, pb, na, nb, fa, fb, out_a, out_b, other_a, other_b, held_ref, stack):
    odd, late = upper(here, axis, 1), upper(here, axis, 2)
    for half, prev, later, far in zip((slice(0, N), slice(N, ROWS)), (pa, pb), (na, nb), (fa, fb)):
        held_ref[0, half, :] = jnp.where(odd, later[...], far[...])
        held_ref[1, half, :] = jnp.where(odd, far[...], prev[...])
    held_ref[3] = own[...]
    swapped = late.astype(jnp.int32)

    def one(k, carry):
        first = held_ref.at[k * (3 - swapped)]
        second = held_ref.at[1 + k * (1 + swapped)]
        done = combine([unpack(*parts(first))], [unpack(*parts(second))], [stack])
        pack(*parts(held_ref.at[2 + 2 * k]), *done[0])
        return carry

    lax.fori_loop(0, 2, one, 0)
    other_a[...] = held_ref[2, 0:N, :]
    other_b[...] = held_ref[2, N:, :]
    out_a[...] = held_ref[4, 0:N, :]
    out_b[...] = held_ref[4, N:, :]


def core_kernel(here, ma, mb, ta, tb, after, out, half, first, second, stack):
    flag = upper(here, "c", 1)
    sort(flag, (ma, mb), (ta, tb), first, second)
    done = combine([unpack(*parts(first))], [unpack(*parts(second))], [stack])
    pack(*parts(out), *done[0])
    half[...] = jnp.where(flag, out[HALF:, :], out[0:HALF, :])


def slow_kernel(axis, step, here, ta, tb, pair, after, out, stack):
    flag = upper(here, axis, step)

    @pl.when(flag)
    def _():
        def one(k, carry):
            done = combine([unpack(ta, tb)], [unpack(*parts(pair.at[k]))], [stack])
            pack(*parts(out.at[k]), *done[0])
            return carry

        lax.fori_loop(0, 2, one, 0)

    @pl.when(jnp.logical_not(flag))
    def _():
        out[...] = pair[...]


def held(here, axes):
    flag = upper(here, *axes[0])
    for axis in axes[1:]:
        flag = jnp.logical_or(flag, upper(here, *axis))
    return flag


Z_LEVEL = (("z", 1), ("z", 2))
CORE_LEVEL = Z_LEVEL + (("c", 1),)


def merge_into(out, has_early, has_late, early, late, stack):
    @pl.when(jnp.logical_and(has_early, has_late))
    def _():
        pack(*parts(out), *combine([unpack(*early)], [unpack(*late)], [stack])[0])

    @pl.when(jnp.logical_not(has_early))
    def _():
        out[0:N, :] = late[0][...]
        out[N:, :] = late[1][...]

    @pl.when(jnp.logical_not(has_late))
    def _():
        out[0:N, :] = early[0][...]
        out[N:, :] = early[1][...]


def ringed_kernel(here, oa, ob, pa, pb, after, out, stack):
    merge_into(out, upper(here, "z", 2), upper(here, "z", 1), (oa, ob), (pa, pb), stack)


def cored_kernel(here, ta, tb, low, after, out, stack):
    merge_into(out, upper(here, "c", 1), held(here, Z_LEVEL), (ta, tb), parts(low), stack)


def steps_kernel(here, theirs, low, pair, after, out, held_ref, stack):
    x_up = upper(here, "x", 1)
    has_low = held(here, CORE_LEVEL)
    held_ref[0] = theirs[...]
    held_ref[1] = low[...]
    held_ref[3:5] = pair[...]
    both = jnp.logical_and(x_up, has_low)
    either = jnp.logical_or(x_up, has_low)
    source = jnp.where(both, 2, jnp.where(has_low, 1, 0))

    def one(k, carry):
        first = held_ref.at[jnp.where(k == 0, 0, source)]
        second = held_ref.at[jnp.where(k == 0, 1, k + 2)]
        done = combine([unpack(*parts(first))], [unpack(*parts(second))], [stack])
        pack(*parts(held_ref.at[k + 2]), *done[0])
        return carry

    lax.fori_loop(jnp.where(both, 0, 1), jnp.where(either, 3, 1), one, 0)
    out[...] = held_ref[3:5]


def is_first(here):
    return (here[0] >> 5) == 0


def prior_kernel(here, whole, mean, cov, mean_out, cov_out, stack):
    @pl.when(is_first(here))
    def _():
        state = jnp.broadcast_to(mean[...], (V, N))
        done = apply_state(state, cov[...], [unpack(*parts(whole))], [stack])
        mean_out[...], cov_out[...] = done[0]

    @pl.when(jnp.logical_not(is_first(here)))
    def _():
        mean_out[...] = jnp.broadcast_to(mean[...], (V, N))
        cov_out[...] = cov[...]


HN = N // 2


def second_kernel(here, mine, other, mean, cov, after, theirs, out, stack):
    flag = upper(here, "c", 1)
    theirs[0:HALF, :] = jnp.where(flag, other[...], mine[...])
    theirs[HALF:, :] = jnp.where(flag, mine[...], other[...])

    @pl.when(is_first(here))
    def _():
        mean_b, cov_b = apply_state(
            mean[...], cov[...], [unpack(*parts(theirs))], [stack]
        )[0]
        row, col = row_col(HN)
        last = cov_b[HN:, HN:]
        out[0:HN, 0:HN] = jnp.where(row <= col, cov_b[0:HN, 0:HN], last)
        out[0:HN, HN:] = cov_b[0:HN, HN:]
        diag = jnp.sum(jnp.where(row == col, last, 0.0), axis=0, keepdims=True)
        out[HN : HN + 8, :] = mean_b[0:8]
        out[HN + 8 :, :] = jnp.broadcast_to(jnp.concatenate([diag, diag], axis=1), (8, N))

    @pl.when(jnp.logical_not(is_first(here)))
    def _():
        out[...] = jnp.zeros((HN + 16, N), F32)


def final_kernel(here, state_a, state_b, mean, cov, pair, means, covs, packed, prior, stack, stack_b):
    packed[...] = jnp.where(upper(here, "x", 1), state_b[...], state_a[...])
    flag = upper(here, "x", 2)
    row, col = row_col(HN)
    mixed = packed[0:HN, 0:HN]
    turned = mixed.T
    side = packed[0:HN, HN:]
    last = jnp.where(
        row == col, packed[HN + 8 : HN + 9, 0:HN], jnp.where(row > col, mixed, turned)
    )
    prior[0:HN, 0:HN] = jnp.where(flag, jnp.where(row <= col, mixed, turned), cov[0:HN, 0:HN])
    prior[0:HN, HN:] = jnp.where(flag, side, cov[0:HN, HN:])
    prior[HN:, 0:HN] = jnp.where(flag, side.T, cov[HN:, 0:HN])
    prior[HN:, HN:] = jnp.where(flag, last, cov[HN:, HN:])
    mean_in = jnp.broadcast_to(jnp.where(flag, packed[HN : HN + 1, :], mean[...]), (V, N))
    seconds = [unpack(*parts(pair.at[k])) for k in range(2)]
    done = apply_state(mean_in, prior[...], seconds, [stack, stack_b])
    for k in range(2):
        means[k : k + 1, :] = done[k][0][0:1]
        covs[k] = done[k][1]


def call(kernel, places, outs, scratch, products):
    spaces = {"s": pltpu.SMEM, "v": pltpu.VMEM, "a": pl.ANY, "h": pltpu.HBM}
    vmem = pl.BlockSpec(memory_space=pltpu.VMEM)
    shapes = [jax.ShapeDtypeStruct(shape, F32) for shape in outs]
    buffers = [pltpu.VMEM(shape, F32) if isinstance(shape, tuple) else shape for shape in scratch]
    return pl.pallas_call(
        kernel,
        out_shape=shapes if len(shapes) > 1 else shapes[0],
        in_specs=[pl.BlockSpec(memory_space=spaces[place]) for place in places],
        out_specs=[vmem] * len(shapes) if len(shapes) > 1 else vmem,
        scratch_shapes=buffers,
        compiler_params=pltpu.CompilerParams(vmem_limit_bytes=24 << 20),
        cost_estimate=pl.CostEstimate(
            flops=products * 6 * N**3, transcendentals=0, bytes_accessed=8 * N * N
        ),
    )


ELEMENT = (ROWS, N)
PAIR = (2, ROWS, N)
MOVE = (N, N)
SIDE = (N + V, N)
HALF = ROWS // 2
STACK = (2 * N, N)
PACKED = (HN + 16, N)


def on_device(transition, observe, noise_obs, measured, noise_state, prior_mean, prior_cov):
    here = lax.axis_index(AXES).astype(jnp.int32)[None]
    mean = prior_mean[None]

    def swap(part, axis, step):
        size = lax.axis_size(axis)
        return lax.ppermute(part, axis, [(k, k ^ step) for k in range(size)])

    def ring(axis, mine, after):
        def turn(part, step):
            return lax.ppermute(part, axis, [(k, (k + step) % 4) for k in range(4)])

        later_a, prev_b = turn(mine[0], 3), turn(mine[1], 1)
        prev_a, later_b = turn(mine[0], 1), turn(mine[1], 3)
        far_a = turn(later_a, 3)
        far_b = turn(prev_b, 1)
        kernel = functools.partial(own_kernel, axis)
        scratch = [ELEMENT, ELEMENT, STACK]
        near = (prev_a, prev_b, later_a, later_b)
        own = call(kernel, "svvvvvva", [ELEMENT], scratch, 14)(here, *mine, *near, after)
        kernel = functools.partial(ring_kernel, axis)
        run = call(kernel, "svvvvvvv", [MOVE, SIDE] * 2, [(5, *ELEMENT), STACK], 28)
        whole_a, whole_b, *other = run(here, own, *near, far_a, far_b)
        return (whole_a, whole_b), (prev_a, prev_b), other

    def slow(axis, step, theirs, pair, after):
        kernel = functools.partial(slow_kernel, axis, step)
        return call(kernel, "svvva", [PAIR], [STACK], 28)(here, *theirs, pair, after)

    ringed = call(ringed_kernel, "svvvva", [ELEMENT], [STACK], 14)
    cored = call(cored_kernel, "svvva", [ELEMENT], [STACK], 14)
    steps = call(steps_kernel, "svvva", [PAIR], [(5, *ELEMENT), STACK], 42)

    inputs = [(2, N, N), (2, O, N), (2, O), (2, O), (N, N)]
    build = call(
        build_kernel,
        "hhhhh",
        [MOVE, SIDE, PAIR],
        inputs + [pltpu.SemaphoreType.DMA((5,)), STACK, (2 * O, O), (2 * O, O)],
        30,
    )
    core = call(core_kernel, "svvvva", [ELEMENT, (HALF, N)], [ELEMENT, ELEMENT, STACK], 14)
    prior = call(prior_kernel, "svvv", [(V, N), (N, N)], [STACK], 14)
    second = call(second_kernel, "svvvva", [ELEMENT, PACKED], [STACK], 14)
    final = call(final_kernel, "svvvvv", [(2, N), (2, N, N)], [PACKED, (N, N), STACK, STACK], 24)

    arrays = (transition, observe, noise_obs, measured, noise_state)
    *whole, pair = build(*(pltpu.with_memory_space_constraint(a, pltpu.HBM) for a in arrays))
    whole, prev, other = ring("y", whole, here)
    pair = slow("y", 1, prev, pair, whole[0])
    pair = slow("y", 2, other, pair, whole[0])
    whole, prev, other = ring("z", whole, pair)
    c1 = [swap(half, "c", 1) for half in whole]
    low = ringed(here, *other, *prev, whole[0])
    whole, half = core(here, *whole, *c1, low)
    x1 = swap(half, "x", 1)
    mean_a, cov_a = prior(here, whole, mean, prior_cov)
    low = cored(here, *c1, low, mean_a)
    x1_other = swap(x1, "c", 1)
    theirs, packed = second(here, x1, x1_other, mean_a, cov_a, low)
    state_a = lax.ppermute(packed, "x", [(0, 2)])
    state_b = lax.ppermute(packed, "x", [(0, 3)])
    pair = steps(here, theirs, low, pair, packed)
    return final(here, state_a, state_b, mean, prior_cov, pair)


def solution(mesh):
    split_mesh = Mesh(mesh.devices.reshape(4, 2, 4, 4), AXES)
    return jax.shard_map(
        on_device,
        mesh=split_mesh,
        in_specs=(
            P(AXES, None, None),
            P(AXES, None, None),
            P(AXES, None),
            P(AXES, None),
            P(),
            P(),
            P(),
        ),
        out_specs=(P(AXES, None), P(AXES, None, None)),
        check_vma=False,
    )
```

```python
import functools

import jax
import jax.numpy as jnp
from jax import lax
from jax.experimental import pallas as pl
from jax.experimental.pallas import tpu as pltpu
from jax.sharding import Mesh
from jax.sharding import PartitionSpec as P


AXES = ("x", "c", "z", "y")
N = 256
O = 64
V = 16
ROWS = 2 * N + V
TOL = 1e-5
F32 = jnp.float32
BF16 = jnp.bfloat16


def split(x):
    high = x.astype(BF16)
    low = (x - high.astype(F32)).astype(BF16)
    return high, low


def dot3(a, b, dims=((1,), (0,))):
    def one(p, q):
        return lax.dot_general(p, q, (dims, ((), ())), preferred_element_type=F32)

    return one(a[0], b[0]) + (one(a[0], b[1]) + one(a[1], b[0]))


def rows(*parts):
    return tuple(jnp.concatenate([p[i] for p in parts], axis=0) for i in range(2))


def row_col(n):
    return (
        lax.broadcasted_iota(jnp.int32, (n, n), 0),
        lax.broadcasted_iota(jnp.int32, (n, n), 1),
    )


def norm(array):
    return jnp.sqrt(jnp.sum(array * array))


def resolvents(coupled, stacks, tight=True):
    n = coupled[0].shape[0]
    row, col = row_col(n)
    eye = jnp.where(row == col, 1.0, 0.0).astype(F32)
    bound = norm(coupled[0])
    for each in coupled[1:]:
        bound = jnp.maximum(bound, norm(each))

    def rate_of(bound):
        return jnp.minimum(bound * bound / (bound * bound + 8.0 * bound + 8.0), 0.9999998)

    def start(bound):
        scale = 1.0 / (bound * bound + 8.0 * bound + 8.0)
        for each, stack in zip(coupled, stacks):
            stack[0:n, :] = (8.0 * scale) * ((bound + 1.0) * eye - each)
        return scale

    loose = rate_of(bound)
    start(bound)

    @pl.when(loose > TOL)
    def _():
        for each, stack in zip(coupled, stacks):
            each2 = split(each)
            stack[n:, :] = dot3(each2, each2)

        def tighten():
            squared = norm(stacks[0][n:, :])
            for stack in stacks[1:]:
                squared = jnp.maximum(squared, norm(stack[n:, :]))
            return jnp.minimum(bound, jnp.sqrt(squared))

        tighter = lax.cond(loose * loose > TOL, tighten, lambda: bound) if tight else bound
        scale = start(tighter)
        for each, stack in zip(coupled, stacks):
            stack[n:, :] = (tighter * tighter * scale) * eye + (8.0 * scale) * (
                stack[n:, :] - tighter * each
            )

        def sweep(rate):
            for stack in stacks:
                both = split(stack[...])
                fresh = dot3(both, (both[0][n:], both[1][n:]))
                stack[0:n, :] = stack[0:n, :] + fresh[0:n]
                stack[n:, :] = fresh[n:]
            return rate * rate

        lax.while_loop(lambda rate: rate > TOL, sweep, rate_of(tighter))

    return [stack[0:n, :] for stack in stacks]


def unpack(move_ref, side_ref):
    both = side_ref[0:N, :]
    vecs = side_ref[N:, :]
    row, col = row_col(N)
    turned = both.T
    spread = jnp.where(row <= col, both, turned)
    info = jnp.where(row == col, vecs[2:3, :], jnp.where(row > col, both, turned))
    return move_ref[...], spread, info, vecs


def pack(move_ref, side_ref, move, spread, info, offset, info_vec):
    row, col = row_col(N)
    move_ref[...] = move
    side_ref[0:N, :] = jnp.where(row <= col, spread, info)
    diag = jnp.sum(jnp.where(row == col, info, 0.0), axis=0, keepdims=True)
    place = lax.broadcasted_iota(jnp.int32, (V, N), 0)
    side_ref[N:, :] = jnp.where(
        place == 0, offset, jnp.where(place == 1, info_vec, jnp.where(place == 2, diag, 0.0))
    )


def parts(ref):
    return ref.at[0:N], ref.at[N:]


def combine(firsts, seconds, stacks, tight=True):
    pairs = []
    for (move_a, spr_a, mat_a, vecs_a), (move_b, spr_b, mat_b, vecs_b) in zip(firsts, seconds):
        move_a2, spr_a2, mat_b2 = split(move_a), split(spr_a), split(mat_b)
        up = dot3(rows(mat_b2, split(vecs_b)), spr_a2)
        seen = dot3(rows(move_a2, split(vecs_a)), mat_b2)
        pairs.append((up, seen, move_a2, spr_a2))
    settled = resolvents([pair[0][0:N] for pair in pairs], stacks, tight)
    out = []
    for first, second, pair, settle in zip(firsts, seconds, pairs, settled):
        up, seen, move_a2, spr_a2 = pair
        move_b, spr_b, _, vecs_b = second
        _, _, mat_a, vecs_a = first
        row_r = vecs_a + up[N + 1 : N + 2]
        row_s = vecs_b[1:2] - seen[N : N + 1]
        third2 = split(dot3(rows(move_a2, spr_a2, split(row_r)), split(settle)))
        fourth = dot3(third2, split(move_b))
        back2 = (third2[0][0:N], third2[1][0:N])
        fifth = dot3(
            rows(split(seen[0:N]), split(jnp.broadcast_to(row_s, (V, N)))), back2, ((1,), (1,))
        )
        spread = dot3(split(move_b.T), split(fourth[N : 2 * N])) + spr_b
        out.append(
            (
                fourth[0:N],
                spread,
                fifth[0:N] + mat_a,
                fourth[2 * N : 2 * N + 1] + vecs_b[0:1],
                fifth[N : N + 1] + vecs_a[1:2],
            )
        )
    return out


def apply_state(mean, cov, seconds, stacks):
    cov2 = split(cov)
    ups = [dot3(rows(split(mat_b), split(vecs_b)), cov2) for _, _, mat_b, vecs_b in seconds]
    settled = resolvents([up[0:N] for up in ups], stacks)
    out = []
    for (move_b, spr_b, _, vecs_b), up, settle in zip(seconds, ups, settled):
        row_r = mean + up[N + 1 : N + 2]
        third = dot3(rows(cov2, split(row_r)), split(settle))
        fourth = dot3(split(third), split(move_b))
        spread = dot3(split(move_b.T), split(fourth[0:N])) + spr_b
        out.append((fourth[N:] + vecs_b[0:1], spread))
    return out


def build_kernel(
    trans_in, obs_in, noise_in, meas_in, state_in, move_ref, side_ref, pair, trans, obs, noise, meas,
    noise_state, sems, stack, small_a, small_b,
):
    copies = [
        pltpu.make_async_copy(source, target, sems.at[k])
        for k, (source, target) in enumerate(
            (
                (obs_in, obs),
                (state_in, noise_state),
                (trans_in, trans),
                (noise_in, noise),
                (meas_in, meas),
            )
        )
    ]
    for copy in copies:
        copy.start()
    for k in (0, 1, 3, 4):
        copies[k].wait()
    state = noise_state[...]
    state2 = split(state)
    place = lax.broadcasted_iota(jnp.int32, (V, N), 0)
    row, col = row_col(O)
    found = []
    sensors = [split(obs[k]) for k in range(2)]
    all_sensed = [dot3(sensor2, state2) for sensor2 in sensors]
    copies[2].wait()
    for k in range(2):
        sensor2, sensed = sensors[k], all_sensed[k]
        seen = dot3(sensor2, split(trans[k]))
        inner = dot3(split(sensed), sensor2, ((1,), (1,)))
        variance = noise[k : k + 1, :]
        root = lax.rsqrt(variance)
        root = root * (1.5 - 0.5 * variance * root * root)
        root_col = jnp.sum(jnp.where(row == col, root, 0.0), axis=1, keepdims=True)
        found.append((sensed, seen, root_col * inner * root, root, root_col))
    inverses = resolvents([part[2] for part in found], (small_a, small_b), False)
    steps = []
    for k in range(2):
        sensed, seen, _, root, root_col = found[k]
        inverse2 = split(root_col * inverses[k] * root)
        pair2 = split(jnp.concatenate([seen, sensed], axis=1))
        solved = dot3(inverse2, pair2)
        value = split(jnp.broadcast_to(meas[k : k + 1, :], (V, O)))
        vec = dot3(split(dot3(value, inverse2)), pair2)
        turned2 = split(jnp.concatenate([seen.T, sensed.T], axis=0))
        full = dot3(turned2, split(solved))
        vecs = jnp.where(place == 0, vec[0:1, N:], jnp.where(place == 1, vec[0:1, 0:N], 0.0))
        steps.append((trans[k].T - full[0:N, N:], state - full[N:, N:], full[0:N, 0:N], vecs))
    move, spread, info, vecs = steps[0]
    pack(*parts(pair.at[0]), move, spread, info, vecs[0:1], vecs[1:2])
    pack(move_ref, side_ref, *combine(steps[0:1], steps[1:2], [stack], False)[0])
    pair[1, 0:N, :] = move_ref[...]
    pair[1, N:, :] = side_ref[...]


def upper(here, axis, step):
    shift = {"x": 5, "c": 4, "z": 2, "y": 0}[axis] + step // 2
    return ((here[0] >> shift) & 1) == 1


def own_kernel(axis, here, ma, mb, pa, pb, na, nb, after, out, first, second, stack):
    odd = upper(here, axis, 1)
    for half, mine, prev, later in zip((slice(0, N), slice(N, ROWS)), (ma, mb), (pa, pb), (na, nb)):
        first[half, :] = jnp.where(odd, prev[...], mine[...])
        second[half, :] = jnp.where(odd, mine[...], later[...])
    done = combine([unpack(*parts(first))], [unpack(*parts(second))], [stack], False)
    pack(*parts(out), *done[0])


def ring_kernel(axis, here, own, pa, pb, na, nb, fa, fb, *refs):
    *out, other_a, other_b, held_ref, stack = refs
    odd, late = upper(here, axis, 1), upper(here, axis, 2)
    for half, prev, later, far in zip((slice(0, N), slice(N, ROWS)), (pa, pb), (na, nb), (fa, fb)):
        held_ref[0, half, :] = jnp.where(odd, later[...], far[...])
        held_ref[1, half, :] = jnp.where(odd, far[...], prev[...])
    held_ref[3] = own[...]
    swapped = late.astype(jnp.int32)

    def one(k, carry):
        first = held_ref.at[k * (3 - swapped)]
        second = held_ref.at[1 + k * (1 + swapped)]
        done = combine([unpack(*parts(first))], [unpack(*parts(second))], [stack], False)
        pack(*parts(held_ref.at[2 + 2 * k]), *done[0])
        return carry

    lax.fori_loop(0, 2, one, 0)
    other_a[...] = held_ref[2, 0:N, :]
    other_b[...] = held_ref[2, N:, :]
    if len(out) == 1:
        out[0][...] = held_ref[4]
    else:
        out[0][...] = held_ref[4, 0:N, :]
        out[1][...] = held_ref[4, N:, :]


def core_kernel(here, mine, theirs, after, out, half, first, second, stack):
    flag = upper(here, "c", 1)
    first[...] = jnp.where(flag, theirs[...], mine[...])
    second[...] = jnp.where(flag, mine[...], theirs[...])
    done = combine([unpack(*parts(first))], [unpack(*parts(second))], [stack], False)
    pack(*parts(out), *done[0])
    half[...] = jnp.where(flag, out[HALF:, :], out[0:HALF, :])


def slow_kernel(step, here, ta, tb, pair, after, out, stack):
    out[...] = pair[...]

    def one(k, carry):
        second = out.at[k]
        done = combine([unpack(ta, tb)], [unpack(*parts(second))], [stack], False)
        pack(*parts(second), *done[0])
        return carry

    lax.fori_loop(0, 2 * upper(here, "y", step).astype(jnp.int32), one, 0)


def held(here, axes):
    flag = upper(here, *axes[0])
    for axis in axes[1:]:
        flag = jnp.logical_or(flag, upper(here, *axis))
    return flag


Z_LEVEL = (("z", 1), ("z", 2))
CORE_LEVEL = Z_LEVEL + (("c", 1),)


def merge_into(out, has_early, has_late, early, late, stack):
    @pl.when(jnp.logical_and(has_early, has_late))
    def _():
        pack(*parts(out), *combine([unpack(*early)], [unpack(*late)], [stack], False)[0])

    @pl.when(jnp.logical_not(has_early))
    def _():
        out[0:N, :] = late[0][...]
        out[N:, :] = late[1][...]

    @pl.when(jnp.logical_not(has_late))
    def _():
        out[0:N, :] = early[0][...]
        out[N:, :] = early[1][...]


def ringed_kernel(here, oa, ob, pa, pb, after, out, stack):
    merge_into(out, upper(here, "z", 2), upper(here, "z", 1), (oa, ob), (pa, pb), stack)


def cored_kernel(here, theirs, low, pair, after, low_out, out, held_ref, stack):
    c_up, has_low = upper(here, "c", 1), held(here, Z_LEVEL)
    held_ref[0] = theirs[...]
    held_ref[1] = low[...]
    held_ref[3:5] = pair[...]
    both = jnp.logical_and(c_up, has_low)
    steps = jnp.logical_and(jnp.logical_or(c_up, has_low), jnp.logical_not(is_first(here)))
    source = jnp.where(both, 2, jnp.where(has_low, 1, 0))

    def one(k, carry):
        first = held_ref.at[jnp.where(k == 0, 0, source)]
        second = held_ref.at[jnp.where(k == 0, 1, k + 2)]
        done = combine([unpack(*parts(first))], [unpack(*parts(second))], [stack], False)
        pack(*parts(held_ref.at[k + 2]), *done[0])
        return carry

    lax.fori_loop(jnp.where(both, 0, 1), jnp.where(steps, 3, 1), one, 0)
    low_out[...] = held_ref[source]
    out[...] = held_ref[3:5]


def steps_kernel(here, theirs, pair, after, out, stack):
    out[...] = pair[...]

    def one(k, carry):
        second = out.at[k]
        done = combine([unpack(*parts(theirs))], [unpack(*parts(second))], [stack])
        pack(*parts(second), *done[0])
        return carry

    lax.fori_loop(0, 2 * upper(here, "x", 1).astype(jnp.int32), one, 0)


def is_first(here):
    return (here[0] >> 5) == 0


def prior_kernel(here, whole, low, mean, cov, means, covs, held_ref, stack):
    state = jnp.broadcast_to(mean[...], (V, N))
    for k, ref in enumerate((whole, low)):
        held_ref[k] = ref[...]
        means[k] = state
        covs[k] = cov[...]

    def one(k, carry):
        done = apply_state(state, cov[...], [unpack(*parts(held_ref.at[k]))], [stack])
        means[k], covs[k] = done[0]
        return carry

    count = 1 + held(here, CORE_LEVEL).astype(jnp.int32)
    lax.fori_loop(0, jnp.where(is_first(here), count, 0), one, 0)


HN = N // 2


def second_kernel(here, mine, other, mean, cov, after, theirs, out, stack):
    flag = upper(here, "c", 1)
    theirs[0:HALF, :] = jnp.where(flag, other[...], mine[...])
    theirs[HALF:, :] = jnp.where(flag, mine[...], other[...])

    @pl.when(is_first(here))
    def _():
        mean_b, cov_b = apply_state(
            mean[0], cov[0], [unpack(*parts(theirs))], [stack]
        )[0]
        row, col = row_col(HN)
        last = cov_b[HN:, HN:]
        out[0:HN, 0:HN] = jnp.where(row <= col, cov_b[0:HN, 0:HN], last)
        out[0:HN, HN:] = cov_b[0:HN, HN:]
        diag = jnp.sum(jnp.where(row == col, last, 0.0), axis=0, keepdims=True)
        out[HN : HN + 8, :] = mean_b[0:8]
        out[HN + 8 :, :] = jnp.broadcast_to(jnp.concatenate([diag, diag], axis=1), (8, N))

    @pl.when(jnp.logical_not(is_first(here)))
    def _():
        out[...] = jnp.zeros((HN + 16, N), F32)


def final_kernel(here, state_a, state_b, mean, cov, pair, means, covs, packed, prior, stack, stack_b):
    packed[...] = jnp.where(upper(here, "x", 1), state_b[...], state_a[...])
    flag = upper(here, "x", 2)
    row, col = row_col(HN)
    mixed = packed[0:HN, 0:HN]
    turned = mixed.T
    side = packed[0:HN, HN:]
    last = jnp.where(
        row == col, packed[HN + 8 : HN + 9, 0:HN], jnp.where(row > col, mixed, turned)
    )
    prior[0:HN, 0:HN] = jnp.where(flag, jnp.where(row <= col, mixed, turned), cov[1, 0:HN, 0:HN])
    prior[0:HN, HN:] = jnp.where(flag, side, cov[1, 0:HN, HN:])
    prior[HN:, 0:HN] = jnp.where(flag, side.T, cov[1, HN:, 0:HN])
    prior[HN:, HN:] = jnp.where(flag, last, cov[1, HN:, HN:])
    mean_in = jnp.broadcast_to(jnp.where(flag, packed[HN : HN + 1, :], mean[1, 0:1, :]), (V, N))
    seconds = [unpack(*parts(pair.at[k])) for k in range(2)]
    done = apply_state(mean_in, prior[...], seconds, [stack, stack_b])
    for k in range(2):
        means[k : k + 1, :] = done[k][0][0:1]
        covs[k] = done[k][1]


def call(kernel, places, outs, scratch, products):
    spaces = {"s": pltpu.SMEM, "v": pltpu.VMEM, "a": pl.ANY, "h": pltpu.HBM}
    vmem = pl.BlockSpec(memory_space=pltpu.VMEM)
    shapes = [jax.ShapeDtypeStruct(shape, F32) for shape in outs]
    buffers = [pltpu.VMEM(shape, F32) if isinstance(shape, tuple) else shape for shape in scratch]
    return pl.pallas_call(
        kernel,
        out_shape=shapes if len(shapes) > 1 else shapes[0],
        in_specs=[pl.BlockSpec(memory_space=spaces[place]) for place in places],
        out_specs=[vmem] * len(shapes) if len(shapes) > 1 else vmem,
        scratch_shapes=buffers,
        compiler_params=pltpu.CompilerParams(vmem_limit_bytes=24 << 20),
        cost_estimate=pl.CostEstimate(
            flops=products * 6 * N**3, transcendentals=0, bytes_accessed=8 * N * N
        ),
    )


ELEMENT = (ROWS, N)
PAIR = (2, ROWS, N)
MOVE = (N, N)
SIDE = (N + V, N)
HALF = ROWS // 2
STACK = (2 * N, N)
PACKED = (HN + 16, N)


def on_device(transition, observe, noise_obs, measured, noise_state, prior_mean, prior_cov):
    here = lax.axis_index(AXES).astype(jnp.int32)[None]
    mean = prior_mean[None]

    def swap(part, axis, step):
        size = lax.axis_size(axis)
        return lax.ppermute(part, axis, [(k, k ^ step) for k in range(size)])

    def ring(axis, mine, after):
        def turn(part, step):
            return lax.ppermute(part, axis, [(k, (k + step) % 4) for k in range(4)])

        later_a, prev_b = turn(mine[0], 3), turn(mine[1], 1)
        prev_a, later_b = turn(mine[0], 1), turn(mine[1], 3)
        far_a = turn(later_a, 3)
        far_b = turn(prev_b, 1)
        kernel = functools.partial(own_kernel, axis)
        scratch = [ELEMENT, ELEMENT, STACK]
        near = (prev_a, prev_b, later_a, later_b)
        own = call(kernel, "svvvvvva", [ELEMENT], scratch, 14)(here, *mine, *near, after)
        kernel = functools.partial(ring_kernel, axis)
        outs = ([MOVE, SIDE] if axis == "y" else [ELEMENT]) + [MOVE, SIDE]
        run = call(kernel, "svvvvvvv", outs, [(5, *ELEMENT), STACK], 28)
        *whole, other_a, other_b = run(here, own, *near, far_a, far_b)
        return whole, (prev_a, prev_b), (other_a, other_b)

    def slow(step, theirs, pair, after):
        kernel = functools.partial(slow_kernel, step)
        return call(kernel, "svvva", [PAIR], [STACK], 28)(here, *theirs, pair, after)

    ringed = call(ringed_kernel, "svvvva", [ELEMENT], [STACK], 14)
    cored = call(cored_kernel, "svvva", [ELEMENT, PAIR], [(5, *ELEMENT), STACK], 42)
    steps = call(steps_kernel, "svva", [PAIR], [STACK], 28)

    inputs = [(2, N, N), (2, O, N), (2, O), (2, O), (N, N)]
    build = call(
        build_kernel,
        "hhhhh",
        [MOVE, SIDE, PAIR],
        inputs + [pltpu.SemaphoreType.DMA((5,)), STACK, (2 * O, O), (2 * O, O)],
        30,
    )
    core = call(core_kernel, "svva", [ELEMENT, (HALF, N)], [ELEMENT, ELEMENT, STACK], 14)
    prior = call(prior_kernel, "svvvv", [(2, V, N), (2, N, N)], [(2, *ELEMENT), STACK], 28)
    second = call(second_kernel, "svvvva", [ELEMENT, PACKED], [STACK], 14)
    final = call(final_kernel, "svvvvv", [(2, N), (2, N, N)], [PACKED, (N, N), STACK, STACK], 24)

    arrays = (transition, observe, noise_obs, measured, noise_state)
    *whole, pair = build(*(pltpu.with_memory_space_constraint(a, pltpu.HBM) for a in arrays))
    whole, prev, other = ring("y", whole, here)
    pair = slow(1, prev, pair, whole[0])
    pair = slow(2, other, pair, whole[0])
    whole, prev, other = ring("z", whole, pair)
    c1 = swap(whole[0], "c", 1)
    low = ringed(here, *other, *prev, whole[0])
    whole, half = core(here, whole[0], c1, low)
    x1 = swap(half, "x", 1)
    low, pair = cored(here, c1, low, pair, whole)
    means, covs = prior(here, whole, low, mean, prior_cov)
    x1_other = swap(x1, "c", 1)
    theirs, packed = second(here, x1, x1_other, means, covs, pair)
    state_a = lax.ppermute(packed, "x", [(0, 2)])
    state_b = lax.ppermute(packed, "x", [(0, 3)])
    pair = steps(here, theirs, pair, packed)
    return final(here, state_a, state_b, means, covs, pair)


def solution(mesh):
    split_mesh = Mesh(mesh.devices.reshape(4, 2, 4, 4), AXES)
    return jax.shard_map(
        on_device,
        mesh=split_mesh,
        in_specs=(
            P(AXES, None, None),
            P(AXES, None, None),
            P(AXES, None),
            P(AXES, None),
            P(),
            P(),
            P(),
        ),
        out_specs=(P(AXES, None), P(AXES, None, None)),
        check_vma=False,
    )
```

```python
import functools

import jax
import jax.numpy as jnp
from jax import lax
from jax.experimental import pallas as pl
from jax.experimental.pallas import tpu as pltpu
from jax.sharding import Mesh
from jax.sharding import PartitionSpec as P


AXES = ("x", "c", "z", "y")
N = 256
O = 64
V = 16
ROWS = 2 * N + V
TOL = 1e-5
F32 = jnp.float32
BF16 = jnp.bfloat16


def split(x):
    high = x.astype(BF16)
    low = (x - high.astype(F32)).astype(BF16)
    return high, low


def dot3(a, b, dims=((1,), (0,))):
    def one(p, q):
        return lax.dot_general(p, q, (dims, ((), ())), preferred_element_type=F32)

    return one(a[0], b[0]) + (one(a[0], b[1]) + one(a[1], b[0]))


def rows(*parts):
    return tuple(jnp.concatenate([p[i] for p in parts], axis=0) for i in range(2))


def row_col(n):
    return (
        lax.broadcasted_iota(jnp.int32, (n, n), 0),
        lax.broadcasted_iota(jnp.int32, (n, n), 1),
    )


def norm(array):
    return jnp.sqrt(jnp.sum(array * array))


def resolvents(coupled, stacks, tight=True):
    n = coupled[0].shape[0]
    row, col = row_col(n)
    eye = jnp.where(row == col, 1.0, 0.0).astype(F32)
    bound = norm(coupled[0])
    for each in coupled[1:]:
        bound = jnp.maximum(bound, norm(each))

    def rate_of(bound):
        return jnp.minimum(bound * bound / (bound * bound + 8.0 * bound + 8.0), 0.9999998)

    def start(bound):
        scale = 1.0 / (bound * bound + 8.0 * bound + 8.0)
        for each, stack in zip(coupled, stacks):
            stack[0:n, :] = (8.0 * scale) * ((bound + 1.0) * eye - each)
        return scale

    loose = rate_of(bound)
    start(bound)

    @pl.when(loose > TOL)
    def _():
        for each, stack in zip(coupled, stacks):
            each2 = split(each)
            stack[n:, :] = dot3(each2, each2)

        def tighten():
            squared = norm(stacks[0][n:, :])
            for stack in stacks[1:]:
                squared = jnp.maximum(squared, norm(stack[n:, :]))
            return jnp.minimum(bound, jnp.sqrt(squared))

        tighter = lax.cond(loose * loose > TOL, tighten, lambda: bound) if tight else bound
        scale = start(tighter)
        for each, stack in zip(coupled, stacks):
            stack[n:, :] = (tighter * tighter * scale) * eye + (8.0 * scale) * (
                stack[n:, :] - tighter * each
            )

        def sweep(rate):
            for stack in stacks:
                both = split(stack[...])
                fresh = dot3(both, (both[0][n:], both[1][n:]))
                stack[0:n, :] = stack[0:n, :] + fresh[0:n]
                stack[n:, :] = fresh[n:]
            return rate * rate

        lax.while_loop(lambda rate: rate > TOL, sweep, rate_of(tighter))

    return [stack[0:n, :] for stack in stacks]


def unpack(move_ref, side_ref):
    both = side_ref[0:N, :]
    vecs = side_ref[N:, :]
    row, col = row_col(N)
    turned = both.T
    spread = jnp.where(row <= col, both, turned)
    info = jnp.where(row == col, vecs[2:3, :], jnp.where(row > col, both, turned))
    return move_ref[...], spread, info, vecs


def pack(move_ref, side_ref, move, spread, info, offset, info_vec):
    row, col = row_col(N)
    move_ref[...] = move
    side_ref[0:N, :] = jnp.where(row <= col, spread, info)
    diag = jnp.sum(jnp.where(row == col, info, 0.0), axis=0, keepdims=True)
    place = lax.broadcasted_iota(jnp.int32, (V, N), 0)
    side_ref[N:, :] = jnp.where(
        place == 0, offset, jnp.where(place == 1, info_vec, jnp.where(place == 2, diag, 0.0))
    )


def parts(ref):
    return ref.at[0:N], ref.at[N:]


def combine(firsts, seconds, stacks, tight=True):
    pairs = []
    for (move_a, spr_a, mat_a, vecs_a), (move_b, spr_b, mat_b, vecs_b) in zip(firsts, seconds):
        move_a2, spr_a2, mat_b2 = split(move_a), split(spr_a), split(mat_b)
        up = dot3(rows(mat_b2, split(vecs_b)), spr_a2)
        seen = dot3(rows(move_a2, split(vecs_a)), mat_b2)
        pairs.append((up, seen, move_a2, spr_a2))
    settled = resolvents([pair[0][0:N] for pair in pairs], stacks, tight)
    out = []
    for first, second, pair, settle in zip(firsts, seconds, pairs, settled):
        up, seen, move_a2, spr_a2 = pair
        move_b, spr_b, _, vecs_b = second
        _, _, mat_a, vecs_a = first
        row_r = vecs_a + up[N + 1 : N + 2]
        row_s = vecs_b[1:2] - seen[N : N + 1]
        third2 = split(dot3(rows(move_a2, spr_a2, split(row_r)), split(settle)))
        move_b2 = split(move_b)
        fourth = dot3(third2, move_b2)
        back2 = (third2[0][0:N], third2[1][0:N])
        fifth = dot3(
            rows(split(seen[0:N]), split(jnp.broadcast_to(row_s, (V, N)))), back2, ((1,), (1,))
        )
        spread = dot3(move_b2, split(fourth[N : 2 * N]), ((0,), (0,))) + spr_b
        out.append(
            (
                fourth[0:N],
                spread,
                fifth[0:N] + mat_a,
                fourth[2 * N : 2 * N + 1] + vecs_b[0:1],
                fifth[N : N + 1] + vecs_a[1:2],
            )
        )
    return out


def apply_state(mean, cov, seconds, stacks):
    cov2 = split(cov)
    ups = [dot3(rows(split(mat_b), split(vecs_b)), cov2) for _, _, mat_b, vecs_b in seconds]
    settled = resolvents([up[0:N] for up in ups], stacks)
    out = []
    for (move_b, spr_b, _, vecs_b), up, settle in zip(seconds, ups, settled):
        row_r = mean + up[N + 1 : N + 2]
        third = dot3(rows(cov2, split(row_r)), split(settle))
        move_b2 = split(move_b)
        fourth = dot3(split(third), move_b2)
        spread = dot3(move_b2, split(fourth[0:N]), ((0,), (0,))) + spr_b
        out.append((fourth[N:] + vecs_b[0:1], spread))
    return out


def build_kernel(
    trans_in, obs_in, noise_in, meas_in, state_in, move_ref, side_ref, pair, trans, obs, noise, meas,
    noise_state, sems, stack, small_a, small_b,
):
    copies = [
        pltpu.make_async_copy(source, target, sems.at[k])
        for k, (source, target) in enumerate(
            (
                (obs_in, obs),
                (state_in, noise_state),
                (trans_in, trans),
                (noise_in, noise),
                (meas_in, meas),
            )
        )
    ]
    for copy in copies:
        copy.start()
    for k in (0, 1, 3, 4):
        copies[k].wait()
    state = noise_state[...]
    state2 = split(state)
    place = lax.broadcasted_iota(jnp.int32, (V, N), 0)
    row, col = row_col(O)
    found = []
    sensors = [split(obs[k]) for k in range(2)]
    all_sensed = [dot3(sensor2, state2) for sensor2 in sensors]
    copies[2].wait()
    for k in range(2):
        sensor2, sensed = sensors[k], all_sensed[k]
        seen = dot3(sensor2, split(trans[k]))
        inner = dot3(split(sensed), sensor2, ((1,), (1,)))
        variance = noise[k : k + 1, :]
        root = lax.rsqrt(variance)
        root = root * (1.5 - 0.5 * variance * root * root)
        root_col = jnp.sum(jnp.where(row == col, root, 0.0), axis=1, keepdims=True)
        found.append((sensed, seen, root_col * inner * root, root, root_col))
    inverses = resolvents([part[2] for part in found], (small_a, small_b), False)
    steps = []
    for k in range(2):
        sensed, seen, _, root, root_col = found[k]
        inverse2 = split(root_col * inverses[k] * root)
        pair2 = split(jnp.concatenate([seen, sensed], axis=1))
        solved = dot3(inverse2, pair2)
        value = split(jnp.broadcast_to(meas[k : k + 1, :], (V, O)))
        vec = dot3(split(dot3(value, inverse2)), pair2)
        turned2 = split(jnp.concatenate([seen.T, sensed.T], axis=0))
        full = dot3(turned2, split(solved))
        vecs = jnp.where(place == 0, vec[0:1, N:], jnp.where(place == 1, vec[0:1, 0:N], 0.0))
        steps.append((trans[k].T - full[0:N, N:], state - full[N:, N:], full[0:N, 0:N], vecs))
    move, spread, info, vecs = steps[0]
    pack(*parts(pair.at[0]), move, spread, info, vecs[0:1], vecs[1:2])
    pack(move_ref, side_ref, *combine(steps[0:1], steps[1:2], [stack], False)[0])
    pair[1, 0:N, :] = move_ref[...]
    pair[1, N:, :] = side_ref[...]


def upper(here, axis, step):
    shift = {"x": 5, "c": 4, "z": 2, "y": 0}[axis] + step // 2
    return ((here[0] >> shift) & 1) == 1


def own_kernel(axis, here, ma, mb, pa, pb, na, nb, after, out, first, second, stack):
    odd = upper(here, axis, 1)
    for half, mine, prev, later in zip((slice(0, N), slice(N, ROWS)), (ma, mb), (pa, pb), (na, nb)):
        first[half, :] = jnp.where(odd, prev[...], mine[...])
        second[half, :] = jnp.where(odd, mine[...], later[...])
    done = combine([unpack(*parts(first))], [unpack(*parts(second))], [stack], False)
    pack(*parts(out), *done[0])


def ring_kernel(axis, here, own, pa, pb, na, nb, fa, fb, *refs):
    *out, other_a, other_b, held_ref, stack = refs
    odd, late = upper(here, axis, 1), upper(here, axis, 2)
    for half, prev, later, far in zip((slice(0, N), slice(N, ROWS)), (pa, pb), (na, nb), (fa, fb)):
        held_ref[0, half, :] = jnp.where(odd, later[...], far[...])
        held_ref[1, half, :] = jnp.where(odd, far[...], prev[...])
    held_ref[3] = own[...]
    swapped = late.astype(jnp.int32)

    def one(k, carry):
        first = held_ref.at[k * (3 - swapped)]
        second = held_ref.at[1 + k * (1 + swapped)]
        done = combine([unpack(*parts(first))], [unpack(*parts(second))], [stack], False)
        pack(*parts(held_ref.at[2 + 2 * k]), *done[0])
        return carry

    lax.fori_loop(0, 2, one, 0)
    other_a[...] = held_ref[2, 0:N, :]
    other_b[...] = held_ref[2, N:, :]
    if len(out) == 1:
        out[0][...] = held_ref[4]
    else:
        out[0][...] = held_ref[4, 0:N, :]
        out[1][...] = held_ref[4, N:, :]


def core_kernel(here, mine, theirs, after, out, half, first, second, stack):
    flag = upper(here, "c", 1)
    first[...] = jnp.where(flag, theirs[...], mine[...])
    second[...] = jnp.where(flag, mine[...], theirs[...])
    done = combine([unpack(*parts(first))], [unpack(*parts(second))], [stack], False)
    pack(*parts(out), *done[0])
    half[...] = jnp.where(flag, out[HALF:, :], out[0:HALF, :])


def slow_kernel(step, here, ta, tb, pair, after, out, stack):
    out[...] = pair[...]

    def one(k, carry):
        second = out.at[k]
        done = combine([unpack(ta, tb)], [unpack(*parts(second))], [stack], False)
        pack(*parts(second), *done[0])
        return carry

    lax.fori_loop(0, 2 * upper(here, "y", step).astype(jnp.int32), one, 0)


def held(here, axes):
    flag = upper(here, *axes[0])
    for axis in axes[1:]:
        flag = jnp.logical_or(flag, upper(here, *axis))
    return flag


Z_LEVEL = (("z", 1), ("z", 2))
CORE_LEVEL = Z_LEVEL + (("c", 1),)


def merge_into(out, has_early, has_late, early, late, stack):
    @pl.when(jnp.logical_and(has_early, has_late))
    def _():
        pack(*parts(out), *combine([unpack(*early)], [unpack(*late)], [stack], False)[0])

    @pl.when(jnp.logical_not(has_early))
    def _():
        out[0:N, :] = late[0][...]
        out[N:, :] = late[1][...]

    @pl.when(jnp.logical_not(has_late))
    def _():
        out[0:N, :] = early[0][...]
        out[N:, :] = early[1][...]


def ringed_kernel(here, oa, ob, pa, pb, after, out, stack):
    merge_into(out, upper(here, "z", 2), upper(here, "z", 1), (oa, ob), (pa, pb), stack)


def cored_kernel(here, theirs, low, pair, after, low_out, out, held_ref, stack):
    c_up, has_low = upper(here, "c", 1), held(here, Z_LEVEL)
    held_ref[0] = theirs[...]
    held_ref[1] = low[...]
    held_ref[3:5] = pair[...]
    both = jnp.logical_and(c_up, has_low)
    steps = jnp.logical_and(jnp.logical_or(c_up, has_low), jnp.logical_not(is_first(here)))
    source = jnp.where(both, 2, jnp.where(has_low, 1, 0))

    def one(k, carry):
        first = held_ref.at[jnp.where(k == 0, 0, source)]
        second = held_ref.at[jnp.where(k == 0, 1, k + 2)]
        done = combine([unpack(*parts(first))], [unpack(*parts(second))], [stack], False)
        pack(*parts(held_ref.at[k + 2]), *done[0])
        return carry

    lax.fori_loop(jnp.where(both, 0, 1), jnp.where(steps, 3, 1), one, 0)
    low_out[...] = held_ref[source]
    out[...] = held_ref[3:5]


def steps_kernel(here, theirs, pair, after, out, stack):
    out[...] = pair[...]

    def one(k, carry):
        second = out.at[k]
        done = combine([unpack(*parts(theirs))], [unpack(*parts(second))], [stack])
        pack(*parts(second), *done[0])
        return carry

    lax.fori_loop(0, 2 * upper(here, "x", 1).astype(jnp.int32), one, 0)


def is_first(here):
    return (here[0] >> 5) == 0


def prior_kernel(here, whole, low, mean, cov, means, covs, held_ref, stack):
    state = jnp.broadcast_to(mean[...], (V, N))
    for k, ref in enumerate((whole, low)):
        held_ref[k] = ref[...]
        means[k] = state
        covs[k] = cov[...]

    def one(k, carry):
        done = apply_state(state, cov[...], [unpack(*parts(held_ref.at[k]))], [stack])
        means[k], covs[k] = done[0]
        return carry

    count = 1 + held(here, CORE_LEVEL).astype(jnp.int32)
    lax.fori_loop(0, jnp.where(is_first(here), count, 0), one, 0)


HN = N // 2


def second_kernel(here, mine, other, mean, cov, after, theirs, out, stack):
    flag = upper(here, "c", 1)
    theirs[0:HALF, :] = jnp.where(flag, other[...], mine[...])
    theirs[HALF:, :] = jnp.where(flag, mine[...], other[...])

    @pl.when(is_first(here))
    def _():
        mean_b, cov_b = apply_state(
            mean[0], cov[0], [unpack(*parts(theirs))], [stack]
        )[0]
        row, col = row_col(HN)
        last = cov_b[HN:, HN:]
        out[0:HN, 0:HN] = jnp.where(row <= col, cov_b[0:HN, 0:HN], last)
        out[0:HN, HN:] = cov_b[0:HN, HN:]
        diag = jnp.sum(jnp.where(row == col, last, 0.0), axis=0, keepdims=True)
        out[HN : HN + 8, :] = mean_b[0:8]
        out[HN + 8 :, :] = jnp.broadcast_to(jnp.concatenate([diag, diag], axis=1), (8, N))

    @pl.when(jnp.logical_not(is_first(here)))
    def _():
        out[...] = jnp.zeros((HN + 16, N), F32)


def final_kernel(here, state_a, state_b, mean, cov, pair, means, covs, packed, prior, stack, stack_b):
    packed[...] = jnp.where(upper(here, "x", 1), state_b[...], state_a[...])
    flag = upper(here, "x", 2)
    row, col = row_col(HN)
    mixed = packed[0:HN, 0:HN]
    turned = mixed.T
    side = packed[0:HN, HN:]
    last = jnp.where(
        row == col, packed[HN + 8 : HN + 9, 0:HN], jnp.where(row > col, mixed, turned)
    )
    prior[0:HN, 0:HN] = jnp.where(flag, jnp.where(row <= col, mixed, turned), cov[1, 0:HN, 0:HN])
    prior[0:HN, HN:] = jnp.where(flag, side, cov[1, 0:HN, HN:])
    prior[HN:, 0:HN] = jnp.where(flag, side.T, cov[1, HN:, 0:HN])
    prior[HN:, HN:] = jnp.where(flag, last, cov[1, HN:, HN:])
    mean_in = jnp.broadcast_to(jnp.where(flag, packed[HN : HN + 1, :], mean[1, 0:1, :]), (V, N))
    seconds = [unpack(*parts(pair.at[k])) for k in range(2)]
    done = apply_state(mean_in, prior[...], seconds, [stack, stack_b])
    for k in range(2):
        means[k : k + 1, :] = done[k][0][0:1]
        covs[k] = done[k][1]


def call(kernel, places, outs, scratch, products):
    spaces = {"s": pltpu.SMEM, "v": pltpu.VMEM, "a": pl.ANY, "h": pltpu.HBM}
    vmem = pl.BlockSpec(memory_space=pltpu.VMEM)
    shapes = [jax.ShapeDtypeStruct(shape, F32) for shape in outs]
    buffers = [pltpu.VMEM(shape, F32) if isinstance(shape, tuple) else shape for shape in scratch]
    return pl.pallas_call(
        kernel,
        out_shape=shapes if len(shapes) > 1 else shapes[0],
        in_specs=[pl.BlockSpec(memory_space=spaces[place]) for place in places],
        out_specs=[vmem] * len(shapes) if len(shapes) > 1 else vmem,
        scratch_shapes=buffers,
        compiler_params=pltpu.CompilerParams(vmem_limit_bytes=24 << 20),
        cost_estimate=pl.CostEstimate(
            flops=products * 6 * N**3, transcendentals=0, bytes_accessed=8 * N * N
        ),
    )


ELEMENT = (ROWS, N)
PAIR = (2, ROWS, N)
MOVE = (N, N)
SIDE = (N + V, N)
HALF = ROWS // 2
STACK = (2 * N, N)
PACKED = (HN + 16, N)


def on_device(transition, observe, noise_obs, measured, noise_state, prior_mean, prior_cov):
    here = lax.axis_index(AXES).astype(jnp.int32)[None]
    mean = prior_mean[None]

    def swap(part, axis, step):
        size = lax.axis_size(axis)
        return lax.ppermute(part, axis, [(k, k ^ step) for k in range(size)])

    def ring(axis, mine, after):
        def turn(part, step):
            return lax.ppermute(part, axis, [(k, (k + step) % 4) for k in range(4)])

        later_a, prev_b = turn(mine[0], 3), turn(mine[1], 1)
        prev_a, later_b = turn(mine[0], 1), turn(mine[1], 3)
        far_a = turn(later_a, 3)
        far_b = turn(prev_b, 1)
        kernel = functools.partial(own_kernel, axis)
        scratch = [ELEMENT, ELEMENT, STACK]
        near = (prev_a, prev_b, later_a, later_b)
        own = call(kernel, "svvvvvva", [ELEMENT], scratch, 14)(here, *mine, *near, after)
        kernel = functools.partial(ring_kernel, axis)
        outs = ([MOVE, SIDE] if axis == "y" else [ELEMENT]) + [MOVE, SIDE]
        run = call(kernel, "svvvvvvv", outs, [(5, *ELEMENT), STACK], 28)
        *whole, other_a, other_b = run(here, own, *near, far_a, far_b)
        return whole, (prev_a, prev_b), (other_a, other_b)

    def slow(step, theirs, pair, after):
        kernel = functools.partial(slow_kernel, step)
        return call(kernel, "svvva", [PAIR], [STACK], 28)(here, *theirs, pair, after)

    ringed = call(ringed_kernel, "svvvva", [ELEMENT], [STACK], 14)
    cored = call(cored_kernel, "svvva", [ELEMENT, PAIR], [(5, *ELEMENT), STACK], 42)
    steps = call(steps_kernel, "svva", [PAIR], [STACK], 28)

    inputs = [(2, N, N), (2, O, N), (2, O), (2, O), (N, N)]
    build = call(
        build_kernel,
        "hhhhh",
        [MOVE, SIDE, PAIR],
        inputs + [pltpu.SemaphoreType.DMA((5,)), STACK, (2 * O, O), (2 * O, O)],
        30,
    )
    core = call(core_kernel, "svva", [ELEMENT, (HALF, N)], [ELEMENT, ELEMENT, STACK], 14)
    prior = call(prior_kernel, "svvvv", [(2, V, N), (2, N, N)], [(2, *ELEMENT), STACK], 28)
    second = call(second_kernel, "svvvva", [ELEMENT, PACKED], [STACK], 14)
    final = call(final_kernel, "svvvvv", [(2, N), (2, N, N)], [PACKED, (N, N), STACK, STACK], 24)

    arrays = (transition, observe, noise_obs, measured, noise_state)
    *whole, pair = build(*(pltpu.with_memory_space_constraint(a, pltpu.HBM) for a in arrays))
    whole, prev, other = ring("y", whole, here)
    pair = slow(1, prev, pair, whole[0])
    pair = slow(2, other, pair, whole[0])
    whole, prev, other = ring("z", whole, pair)
    c1 = swap(whole[0], "c", 1)
    low = ringed(here, *other, *prev, whole[0])
    whole, half = core(here, whole[0], c1, low)
    x1 = swap(half, "x", 1)
    low, pair = cored(here, c1, low, pair, whole)
    means, covs = prior(here, whole, low, mean, prior_cov)
    x1_other = swap(x1, "c", 1)
    theirs, packed = second(here, x1, x1_other, means, covs, pair)
    state_a = lax.ppermute(packed, "x", [(0, 2)])
    state_b = lax.ppermute(packed, "x", [(0, 3)])
    pair = steps(here, theirs, pair, packed)
    return final(here, state_a, state_b, means, covs, pair)


def solution(mesh):
    split_mesh = Mesh(mesh.devices.reshape(4, 2, 4, 4), AXES)
    return jax.shard_map(
        on_device,
        mesh=split_mesh,
        in_specs=(
            P(AXES, None, None),
            P(AXES, None, None),
            P(AXES, None),
            P(AXES, None),
            P(),
            P(),
            P(),
        ),
        out_specs=(P(AXES, None), P(AXES, None, None)),
        check_vma=False,
    )
```

```python
import functools

import jax
import jax.numpy as jnp
from jax import lax
from jax.experimental import pallas as pl
from jax.experimental.pallas import tpu as pltpu
from jax.sharding import Mesh
from jax.sharding import PartitionSpec as P


AXES = ("x", "c", "z", "y")
N = 256
O = 64
V = 16
ROWS = 2 * N + V
TOL = 1e-5
F32 = jnp.float32
BF16 = jnp.bfloat16


def split(x):
    high = x.astype(BF16)
    low = (x - high.astype(F32)).astype(BF16)
    return high, low


def dot3(a, b, dims=((1,), (0,))):
    def one(p, q):
        return lax.dot_general(p, q, (dims, ((), ())), preferred_element_type=F32)

    return one(a[0], b[0]) + (one(a[0], b[1]) + one(a[1], b[0]))


def rows(*parts):
    return tuple(jnp.concatenate([p[i] for p in parts], axis=0) for i in range(2))


def row_col(n):
    return (
        lax.broadcasted_iota(jnp.int32, (n, n), 0),
        lax.broadcasted_iota(jnp.int32, (n, n), 1),
    )


def norm(array):
    return jnp.sqrt(jnp.sum(array * array))


def resolvents(coupled, stacks, tight=True):
    n = coupled[0].shape[0]
    row, col = row_col(n)
    eye = jnp.where(row == col, 1.0, 0.0).astype(F32)
    bound = norm(coupled[0])
    for each in coupled[1:]:
        bound = jnp.maximum(bound, norm(each))

    def rate_of(bound):
        return jnp.minimum(bound * bound / (bound * bound + 8.0 * bound + 8.0), 0.9999998)

    def start(bound):
        scale = 1.0 / (bound * bound + 8.0 * bound + 8.0)
        for each, stack in zip(coupled, stacks):
            stack[0:n, :] = (8.0 * scale) * ((bound + 1.0) * eye - each)
        return scale

    loose = rate_of(bound)
    start(bound)

    @pl.when(loose > TOL)
    def _():
        for each, stack in zip(coupled, stacks):
            each2 = split(each)
            stack[n:, :] = dot3(each2, each2)

        def tighten():
            squared = norm(stacks[0][n:, :])
            for stack in stacks[1:]:
                squared = jnp.maximum(squared, norm(stack[n:, :]))
            return jnp.minimum(bound, jnp.sqrt(squared))

        tighter = lax.cond(loose * loose > TOL, tighten, lambda: bound) if tight else bound
        scale = start(tighter)
        for each, stack in zip(coupled, stacks):
            stack[n:, :] = (tighter * tighter * scale) * eye + (8.0 * scale) * (
                stack[n:, :] - tighter * each
            )

        def sweep(rate):
            for stack in stacks:
                both = split(stack[...])
                fresh = dot3(both, (both[0][n:], both[1][n:]))
                stack[0:n, :] = stack[0:n, :] + fresh[0:n]
                stack[n:, :] = fresh[n:]
            return rate * rate

        lax.while_loop(lambda rate: rate > TOL, sweep, rate_of(tighter))

    return [stack[0:n, :] for stack in stacks]


def unpack(move_ref, side_ref):
    both = side_ref[0:N, :]
    vecs = side_ref[N:, :]
    row, col = row_col(N)
    turned = both.T
    spread = jnp.where(row <= col, both, turned)
    info = jnp.where(row == col, vecs[2:3, :], jnp.where(row > col, both, turned))
    return move_ref[...], spread, info, vecs


def pack(move_ref, side_ref, move, spread, info, offset, info_vec):
    row, col = row_col(N)
    move_ref[...] = move
    side_ref[0:N, :] = jnp.where(row <= col, spread, info)
    diag = jnp.sum(jnp.where(row == col, info, 0.0), axis=0, keepdims=True)
    place = lax.broadcasted_iota(jnp.int32, (V, N), 0)
    side_ref[N:, :] = jnp.where(
        place == 0, offset, jnp.where(place == 1, info_vec, jnp.where(place == 2, diag, 0.0))
    )


def parts(ref):
    return ref.at[0:N], ref.at[N:]


def combine(firsts, seconds, stacks, tight=True):
    pairs = []
    for (move_a, spr_a, mat_a, vecs_a), (move_b, spr_b, mat_b, vecs_b) in zip(firsts, seconds):
        move_a2, spr_a2, mat_b2 = split(move_a), split(spr_a), split(mat_b)
        up = dot3(rows(mat_b2, split(vecs_b)), spr_a2)
        seen = dot3(rows(move_a2, split(vecs_a)), mat_b2)
        pairs.append((up, seen, move_a2, spr_a2))
    settled = resolvents([pair[0][0:N] for pair in pairs], stacks, tight)
    out = []
    for first, second, pair, settle in zip(firsts, seconds, pairs, settled):
        up, seen, move_a2, spr_a2 = pair
        move_b, spr_b, _, vecs_b = second
        _, _, mat_a, vecs_a = first
        row_r = vecs_a + up[N + 1 : N + 2]
        row_s = vecs_b[1:2] - seen[N : N + 1]
        third2 = split(dot3(rows(move_a2, spr_a2, split(row_r)), split(settle)))
        move_b2 = split(move_b)
        fourth = dot3(third2, move_b2)
        back2 = (third2[0][0:N], third2[1][0:N])
        fifth = dot3(
            rows(split(seen[0:N]), split(jnp.broadcast_to(row_s, (V, N)))), back2, ((1,), (1,))
        )
        spread = dot3(move_b2, split(fourth[N : 2 * N]), ((0,), (0,))) + spr_b
        out.append(
            (
                fourth[0:N],
                spread,
                fifth[0:N] + mat_a,
                fourth[2 * N : 2 * N + 1] + vecs_b[0:1],
                fifth[N : N + 1] + vecs_a[1:2],
            )
        )
    return out


def apply_state(mean, cov, seconds, stacks):
    cov2 = split(cov)
    ups = [dot3(rows(split(mat_b), split(vecs_b)), cov2) for _, _, mat_b, vecs_b in seconds]
    settled = resolvents([up[0:N] for up in ups], stacks)
    out = []
    for (move_b, spr_b, _, vecs_b), up, settle in zip(seconds, ups, settled):
        row_r = mean + up[N + 1 : N + 2]
        third = dot3(rows(cov2, split(row_r)), split(settle))
        move_b2 = split(move_b)
        fourth = dot3(split(third), move_b2)
        spread = dot3(move_b2, split(fourth[0:N]), ((0,), (0,))) + spr_b
        out.append((fourth[N:] + vecs_b[0:1], spread))
    return out


def build_kernel(
    trans_in, obs_in, noise_in, meas_in, state_in, move_ref, side_ref, one_ref, trans, obs, noise, meas,
    noise_state, sems, stack, small_a, small_b,
):
    copies = [
        pltpu.make_async_copy(source, target, sems.at[k])
        for k, (source, target) in enumerate(
            (
                (obs_in, obs),
                (state_in, noise_state),
                (trans_in, trans),
                (noise_in, noise),
                (meas_in, meas),
            )
        )
    ]
    for copy in copies:
        copy.start()
    for k in (0, 1, 3, 4):
        copies[k].wait()
    state = noise_state[...]
    state2 = split(state)
    place = lax.broadcasted_iota(jnp.int32, (V, N), 0)
    row, col = row_col(O)
    found = []
    sensors = [split(obs[k]) for k in range(2)]
    all_sensed = [dot3(sensor2, state2) for sensor2 in sensors]
    copies[2].wait()
    for k in range(2):
        sensor2, sensed = sensors[k], all_sensed[k]
        seen = dot3(sensor2, split(trans[k]))
        inner = dot3(split(sensed), sensor2, ((1,), (1,)))
        variance = noise[k : k + 1, :]
        root = lax.rsqrt(variance)
        root = root * (1.5 - 0.5 * variance * root * root)
        root_col = jnp.sum(jnp.where(row == col, root, 0.0), axis=1, keepdims=True)
        found.append((sensed, seen, root_col * inner * root, root, root_col))
    inverses = resolvents([part[2] for part in found], (small_a, small_b), False)
    steps = []
    for k in range(2):
        sensed, seen, _, root, root_col = found[k]
        inverse2 = split(root_col * inverses[k] * root)
        pair2 = split(jnp.concatenate([seen, sensed], axis=1))
        solved = dot3(inverse2, pair2)
        value = split(jnp.broadcast_to(meas[k : k + 1, :], (V, O)))
        vec = dot3(split(dot3(value, inverse2)), pair2)
        turned2 = split(jnp.concatenate([seen.T, sensed.T], axis=0))
        full = dot3(turned2, split(solved))
        vecs = jnp.where(place == 0, vec[0:1, N:], jnp.where(place == 1, vec[0:1, 0:N], 0.0))
        steps.append((trans[k].T - full[0:N, N:], state - full[N:, N:], full[0:N, 0:N], vecs))
    move, spread, info, vecs = steps[0]
    pack(*parts(one_ref), move, spread, info, vecs[0:1], vecs[1:2])
    pack(move_ref, side_ref, *combine(steps[0:1], steps[1:2], [stack], False)[0])


def upper(here, axis, step):
    shift = {"x": 5, "c": 4, "z": 2, "y": 0}[axis] + step // 2
    return ((here[0] >> shift) & 1) == 1


def own_kernel(axis, here, ma, mb, pa, pb, na, nb, after, out, first, second, stack):
    odd = upper(here, axis, 1)
    for half, mine, prev, later in zip((slice(0, N), slice(N, ROWS)), (ma, mb), (pa, pb), (na, nb)):
        first[half, :] = jnp.where(odd, prev[...], mine[...])
        second[half, :] = jnp.where(odd, mine[...], later[...])
    done = combine([unpack(*parts(first))], [unpack(*parts(second))], [stack], False)
    pack(*parts(out), *done[0])


def ring_kernel(axis, here, own, pa, pb, na, nb, fa, fb, *refs):
    *out, other_a, other_b, held_ref, stack = refs
    odd, late = upper(here, axis, 1), upper(here, axis, 2)
    for half, prev, later, far in zip((slice(0, N), slice(N, ROWS)), (pa, pb), (na, nb), (fa, fb)):
        held_ref[0, half, :] = jnp.where(odd, later[...], far[...])
        held_ref[1, half, :] = jnp.where(odd, far[...], prev[...])
    held_ref[3] = own[...]
    swapped = late.astype(jnp.int32)

    def one(k, carry):
        first = held_ref.at[k * (3 - swapped)]
        second = held_ref.at[1 + k * (1 + swapped)]
        done = combine([unpack(*parts(first))], [unpack(*parts(second))], [stack], False)
        pack(*parts(held_ref.at[2 + 2 * k]), *done[0])
        return carry

    lax.fori_loop(0, 2, one, 0)
    other_a[...] = held_ref[2, 0:N, :]
    other_b[...] = held_ref[2, N:, :]
    if len(out) == 1:
        out[0][...] = held_ref[4]
    else:
        out[0][...] = held_ref[4, 0:N, :]
        out[1][...] = held_ref[4, N:, :]


def choose(flag, yes, no):
    return tuple(jnp.where(flag, p, q) for p, q in zip(yes, no))


def core_kernel(here, mine, theirs, after, out, half, stack):
    flag = upper(here, "c", 1)
    own, rest = unpack(*parts(mine)), unpack(*parts(theirs))
    done = combine([choose(flag, rest, own)], [choose(flag, own, rest)], [stack], False)
    pack(*parts(out), *done[0])
    half[...] = jnp.where(flag, out[HALF:, :], out[0:HALF, :])


def slow_kernel(step, here, ta, tb, *refs):
    *pair, _, out, stack = refs
    if len(pair) == 1:
        out[...] = pair[0][...]
    else:
        out[0] = pair[0][...]
        out[1, 0:N, :] = pair[1][...]
        out[1, N:, :] = pair[2][...]

    def one(k, carry):
        second = out.at[k]
        done = combine([unpack(ta, tb)], [unpack(*parts(second))], [stack], False)
        pack(*parts(second), *done[0])
        return carry

    lax.fori_loop(0, 2 * upper(here, "y", step).astype(jnp.int32), one, 0)


def held(here, axes):
    flag = upper(here, *axes[0])
    for axis in axes[1:]:
        flag = jnp.logical_or(flag, upper(here, *axis))
    return flag


Z_LEVEL = (("z", 1), ("z", 2))
CORE_LEVEL = Z_LEVEL + (("c", 1),)


def merge_into(out, has_early, has_late, early, late, stack):
    @pl.when(jnp.logical_and(has_early, has_late))
    def _():
        pack(*parts(out), *combine([unpack(*early)], [unpack(*late)], [stack], False)[0])

    @pl.when(jnp.logical_not(has_early))
    def _():
        out[0:N, :] = late[0][...]
        out[N:, :] = late[1][...]

    @pl.when(jnp.logical_not(has_late))
    def _():
        out[0:N, :] = early[0][...]
        out[N:, :] = early[1][...]


def ringed_kernel(here, oa, ob, pa, pb, after, out, stack):
    merge_into(out, upper(here, "z", 2), upper(here, "z", 1), (oa, ob), (pa, pb), stack)


def cored_kernel(here, theirs, low, pair, after, low_out, out, held_ref, stack):
    c_up, has_low = upper(here, "c", 1), held(here, Z_LEVEL)
    held_ref[0] = theirs[...]
    held_ref[1] = low[...]
    held_ref[3:5] = pair[...]
    both = jnp.logical_and(c_up, has_low)
    steps = jnp.logical_and(jnp.logical_or(c_up, has_low), jnp.logical_not(is_first(here)))
    source = jnp.where(both, 2, jnp.where(has_low, 1, 0))

    def one(k, carry):
        first = held_ref.at[jnp.where(k == 0, 0, source)]
        second = held_ref.at[jnp.where(k == 0, 1, k + 2)]
        done = combine([unpack(*parts(first))], [unpack(*parts(second))], [stack], False)
        pack(*parts(held_ref.at[k + 2]), *done[0])
        return carry

    lax.fori_loop(jnp.where(both, 0, 1), jnp.where(steps, 3, 1), one, 0)
    low_out[...] = held_ref[source]
    out[...] = held_ref[3:5]


def steps_kernel(here, theirs, pair, after, out, stack):
    out[...] = pair[...]

    def one(k, carry):
        second = out.at[k]
        done = combine([unpack(*parts(theirs))], [unpack(*parts(second))], [stack])
        pack(*parts(second), *done[0])
        return carry

    lax.fori_loop(0, 2 * upper(here, "x", 1).astype(jnp.int32), one, 0)


def is_first(here):
    return (here[0] >> 5) == 0


def prior_kernel(here, whole, low, mean, cov, means, covs, held_ref, stack):
    state = jnp.broadcast_to(mean[...], (V, N))
    for k, ref in enumerate((whole, low)):
        held_ref[k] = ref[...]
        means[k] = state
        covs[k] = cov[...]

    def one(k, carry):
        done = apply_state(state, cov[...], [unpack(*parts(held_ref.at[k]))], [stack])
        means[k], covs[k] = done[0]
        return carry

    count = 1 + held(here, CORE_LEVEL).astype(jnp.int32)
    lax.fori_loop(0, jnp.where(is_first(here), count, 0), one, 0)


HN = N // 2


def second_kernel(here, mine, other, mean, cov, after, theirs, out, stack):
    flag = upper(here, "c", 1)
    theirs[0:HALF, :] = jnp.where(flag, other[...], mine[...])
    theirs[HALF:, :] = jnp.where(flag, mine[...], other[...])

    @pl.when(is_first(here))
    def _():
        mean_b, cov_b = apply_state(
            mean[0], cov[0], [unpack(*parts(theirs))], [stack]
        )[0]
        row, col = row_col(HN)
        last = cov_b[HN:, HN:]
        out[0:HN, 0:HN] = jnp.where(row <= col, cov_b[0:HN, 0:HN], last)
        out[0:HN, HN:] = cov_b[0:HN, HN:]
        diag = jnp.sum(jnp.where(row == col, last, 0.0), axis=0, keepdims=True)
        out[HN : HN + 8, :] = mean_b[0:8]
        out[HN + 8 :, :] = jnp.broadcast_to(jnp.concatenate([diag, diag], axis=1), (8, N))

    @pl.when(jnp.logical_not(is_first(here)))
    def _():
        out[...] = jnp.zeros((HN + 16, N), F32)


def final_kernel(here, state_a, state_b, mean, cov, pair, means, covs, packed, prior, stack, stack_b):
    packed[...] = jnp.where(upper(here, "x", 1), state_b[...], state_a[...])
    flag = upper(here, "x", 2)
    row, col = row_col(HN)
    mixed = packed[0:HN, 0:HN]
    turned = mixed.T
    side = packed[0:HN, HN:]
    last = jnp.where(
        row == col, packed[HN + 8 : HN + 9, 0:HN], jnp.where(row > col, mixed, turned)
    )
    prior[0:HN, 0:HN] = jnp.where(flag, jnp.where(row <= col, mixed, turned), cov[1, 0:HN, 0:HN])
    prior[0:HN, HN:] = jnp.where(flag, side, cov[1, 0:HN, HN:])
    prior[HN:, 0:HN] = jnp.where(flag, side.T, cov[1, HN:, 0:HN])
    prior[HN:, HN:] = jnp.where(flag, last, cov[1, HN:, HN:])
    mean_in = jnp.broadcast_to(jnp.where(flag, packed[HN : HN + 1, :], mean[1, 0:1, :]), (V, N))
    seconds = [unpack(*parts(pair.at[k])) for k in range(2)]
    done = apply_state(mean_in, prior[...], seconds, [stack, stack_b])
    for k in range(2):
        means[k : k + 1, :] = done[k][0][0:1]
        covs[k] = done[k][1]


def call(kernel, places, outs, scratch, products):
    spaces = {"s": pltpu.SMEM, "v": pltpu.VMEM, "a": pl.ANY, "h": pltpu.HBM}
    vmem = pl.BlockSpec(memory_space=pltpu.VMEM)
    shapes = [jax.ShapeDtypeStruct(shape, F32) for shape in outs]
    buffers = [pltpu.VMEM(shape, F32) if isinstance(shape, tuple) else shape for shape in scratch]
    return pl.pallas_call(
        kernel,
        out_shape=shapes if len(shapes) > 1 else shapes[0],
        in_specs=[pl.BlockSpec(memory_space=spaces[place]) for place in places],
        out_specs=[vmem] * len(shapes) if len(shapes) > 1 else vmem,
        scratch_shapes=buffers,
        compiler_params=pltpu.CompilerParams(vmem_limit_bytes=24 << 20),
        cost_estimate=pl.CostEstimate(
            flops=products * 6 * N**3, transcendentals=0, bytes_accessed=8 * N * N
        ),
    )


ELEMENT = (ROWS, N)
PAIR = (2, ROWS, N)
MOVE = (N, N)
SIDE = (N + V, N)
HALF = ROWS // 2
STACK = (2 * N, N)
PACKED = (HN + 16, N)


def on_device(transition, observe, noise_obs, measured, noise_state, prior_mean, prior_cov):
    here = lax.axis_index(AXES).astype(jnp.int32)[None]
    mean = prior_mean[None]

    def swap(part, axis, step):
        size = lax.axis_size(axis)
        return lax.ppermute(part, axis, [(k, k ^ step) for k in range(size)])

    def ring(axis, mine, after):
        def turn(part, step):
            return lax.ppermute(part, axis, [(k, (k + step) % 4) for k in range(4)])

        later_a, prev_b = turn(mine[0], 3), turn(mine[1], 1)
        prev_a, later_b = turn(mine[0], 1), turn(mine[1], 3)
        far_a = turn(later_a, 3)
        far_b = turn(prev_b, 1)
        kernel = functools.partial(own_kernel, axis)
        scratch = [ELEMENT, ELEMENT, STACK]
        near = (prev_a, prev_b, later_a, later_b)
        own = call(kernel, "svvvvvva", [ELEMENT], scratch, 14)(here, *mine, *near, after)
        kernel = functools.partial(ring_kernel, axis)
        outs = ([MOVE, SIDE] if axis == "y" else [ELEMENT]) + [MOVE, SIDE]
        run = call(kernel, "svvvvvvv", outs, [(5, *ELEMENT), STACK], 28)
        *whole, other_a, other_b = run(here, own, *near, far_a, far_b)
        return whole, (prev_a, prev_b), (other_a, other_b)

    def slow(step, theirs, pair, after):
        kernel = functools.partial(slow_kernel, step)
        places = "svv" + "v" * len(pair) + "a"
        return call(kernel, places, [PAIR], [STACK], 28)(here, *theirs, *pair, after)

    ringed = call(ringed_kernel, "svvvva", [ELEMENT], [STACK], 14)
    cored = call(cored_kernel, "svvva", [ELEMENT, PAIR], [(5, *ELEMENT), STACK], 42)
    steps = call(steps_kernel, "svva", [PAIR], [STACK], 28)

    inputs = [(2, N, N), (2, O, N), (2, O), (2, O), (N, N)]
    build = call(
        build_kernel,
        "hhhhh",
        [MOVE, SIDE, ELEMENT],
        inputs + [pltpu.SemaphoreType.DMA((5,)), STACK, (2 * O, O), (2 * O, O)],
        30,
    )
    core = call(core_kernel, "svva", [ELEMENT, (HALF, N)], [STACK], 14)
    prior = call(prior_kernel, "svvvv", [(2, V, N), (2, N, N)], [(2, *ELEMENT), STACK], 28)
    second = call(second_kernel, "svvvva", [ELEMENT, PACKED], [STACK], 14)
    final = call(final_kernel, "svvvvv", [(2, N), (2, N, N)], [PACKED, (N, N), STACK, STACK], 24)

    arrays = (transition, observe, noise_obs, measured, noise_state)
    *whole, one = build(*(pltpu.with_memory_space_constraint(a, pltpu.HBM) for a in arrays))
    steps_two = tuple(whole)
    whole, prev, other = ring("y", whole, here)
    pair = slow(1, prev, (one, *steps_two), whole[0])
    pair = slow(2, other, (pair,), whole[0])
    whole, prev, other = ring("z", whole, pair)
    c1 = swap(whole[0], "c", 1)
    low = ringed(here, *other, *prev, whole[0])
    whole, half = core(here, whole[0], c1, low)
    x1 = swap(half, "x", 1)
    low, pair = cored(here, c1, low, pair, whole)
    means, covs = prior(here, whole, low, mean, prior_cov)
    x1_other = swap(x1, "c", 1)
    theirs, packed = second(here, x1, x1_other, means, covs, pair)
    state_a = lax.ppermute(packed, "x", [(0, 2)])
    state_b = lax.ppermute(packed, "x", [(0, 3)])
    pair = steps(here, theirs, pair, packed)
    return final(here, state_a, state_b, means, covs, pair)


def solution(mesh):
    split_mesh = Mesh(mesh.devices.reshape(4, 2, 4, 4), AXES)
    return jax.shard_map(
        on_device,
        mesh=split_mesh,
        in_specs=(
            P(AXES, None, None),
            P(AXES, None, None),
            P(AXES, None),
            P(AXES, None),
            P(),
            P(),
            P(),
        ),
        out_specs=(P(AXES, None), P(AXES, None, None)),
        check_vma=False,
    )
```
